8 devices in a mesh: data: 1 (over z), dap: 8 (over y, x, core).
Axes of the slice: x: 2, y: 2, z: 1, core: 2. Of those that a mesh axis runs over, the one named last changes fastest.
Arguments:
- msa_act: bfloat16 [256, 64, 64], P(('data', 'dap'))
- pair_act: bfloat16 [64, 64, 128], P(('data', 'dap'))
- msa_mask: int32 [256, 64], P('data')
- res_mask: int32 [64], P('data')
- w_row_bias: bfloat16 [2, 128, 8], replicated
- w_row_in: bfloat16 [2, 64, 4, 8, 8], replicated
- w_row_out: bfloat16 [2, 8, 8, 64], replicated
- w_col_in: bfloat16 [2, 64, 4, 8, 8], replicated
- w_col_out: bfloat16 [2, 8, 8, 64], replicated
- w_opm_in: bfloat16 [2, 64, 2, 32], replicated
- w_opm_out: bfloat16 [2, 32, 32, 128], replicated
- w_ts_bias: bfloat16 [2, 128, 4], replicated
- w_ts_in: bfloat16 [2, 128, 4, 4, 32], replicated
- w_ts_out: bfloat16 [2, 4, 32, 128], replicated
- w_te_bias: bfloat16 [2, 128, 4], replicated
- w_te_in: bfloat16 [2, 128, 4, 4, 32], replicated
- w_te_out: bfloat16 [2, 4, 32, 128], replicated
Outputs:
- output 1: bfloat16 [256, 64, 64], P(('data', 'dap'))
- output 2: bfloat16 [64, 64, 128], P(('data', 'dap'))
All inputs are finite; a program needn't handle non-finite values.
Results may differ from the reference program's by a relative error of at most 0.0187346.
Values are sent between devices in bfloat16 or wider.
A program may use at most 1 GiB of HBM per device.

```python
import jax
import jax.numpy as jnp
from jax import lax

NR = 64
NS = 256
C_M = 64
C_Z = 128
HEADS_MSA = 8
HEAD_MSA = 8
HEADS_TRI = 4
HEAD_TRI = 32
OPM_DIM = 32


def draw_normal(key, shape, scale):
    return (jax.random.normal(key, shape, jnp.float32) * scale).astype(jnp.bfloat16)


def setup_inputs(seed: int = 0, part: int = 0) -> dict:
    base_key = jax.random.key(seed)
    part_keys = jax.random.split(jax.random.fold_in(base_key, part), 4)
    w_keys = jax.random.split(jax.random.fold_in(base_key, 1000), 13)
    width_msa = HEADS_MSA * HEAD_MSA
    width_tri = HEADS_TRI * HEAD_TRI
    return {
        'msa_act': draw_normal(part_keys[0], (NS, NR, C_M), 1.0),
        'pair_act': draw_normal(part_keys[1], (NR, NR, C_Z), 1.0),
        'msa_mask': (jax.random.randint(part_keys[2], (NS, NR), 0, 4) > 0).astype(jnp.int32),
        'res_mask': (jax.random.randint(part_keys[3], (NR,), 0, 4) > 0).astype(jnp.int32),
        'w_row_bias': draw_normal(w_keys[0], (2, C_Z, HEADS_MSA), 1.5 * C_Z ** -0.5),
        'w_row_in': draw_normal(w_keys[1], (2, C_M, 4, HEADS_MSA, HEAD_MSA), 1.25 * C_M ** -0.5),
        'w_row_out': draw_normal(w_keys[2], (2, HEADS_MSA, HEAD_MSA, C_M), 0.5 * width_msa ** -0.5),
        'w_col_in': draw_normal(w_keys[3], (2, C_M, 4, HEADS_MSA, HEAD_MSA), 1.25 * C_M ** -0.5),
        'w_col_out': draw_normal(w_keys[4], (2, HEADS_MSA, HEAD_MSA, C_M), 0.5 * width_msa ** -0.5),
        'w_opm_in': draw_normal(w_keys[5], (2, C_M, 2, OPM_DIM), C_M ** -0.5),
        'w_opm_out': draw_normal(w_keys[6], (2, OPM_DIM, OPM_DIM, C_Z), 0.25 * NS ** 0.5 / OPM_DIM),
        'w_ts_bias': draw_normal(w_keys[7], (2, C_Z, HEADS_TRI), 1.5 * C_Z ** -0.5),
        'w_ts_in': draw_normal(w_keys[8], (2, C_Z, 4, HEADS_TRI, HEAD_TRI), 1.25 * C_Z ** -0.5),
        'w_ts_out': draw_normal(w_keys[9], (2, HEADS_TRI, HEAD_TRI, C_Z), 0.5 * width_tri ** -0.5),
        'w_te_bias': draw_normal(w_keys[10], (2, C_Z, HEADS_TRI), 1.5 * C_Z ** -0.5),
        'w_te_in': draw_normal(w_keys[11], (2, C_Z, 4, HEADS_TRI, HEAD_TRI), 1.25 * C_Z ** -0.5),
        'w_te_out': draw_normal(w_keys[12], (2, HEADS_TRI, HEAD_TRI, C_Z), 0.5 * width_tri ** -0.5),
    }


def layer_norm(values):
    flat = values.astype(jnp.float32)
    row_mean = jnp.mean(flat, axis=-1, keepdims=True)
    centered = flat - row_mean
    row_var = jnp.mean(centered * centered, axis=-1, keepdims=True)
    return (centered * lax.rsqrt(row_var + 1e-5)).astype(jnp.bfloat16)


def add_residual(current, update):
    return (current.astype(jnp.float32) + update).astype(jnp.bfloat16)


def pair_bias(pair_ln, w_bias):
    num_res = pair_ln.shape[0]
    flat = jnp.dot(pair_ln.reshape(num_res * num_res, -1), w_bias, preferred_element_type=jnp.float32)
    return jnp.transpose(flat.astype(jnp.bfloat16).reshape(num_res, num_res, -1), (2, 0, 1))


def attend_one(x_ln, w_in, w_out, bias_hqk, key_mask):
    length = x_ln.shape[0]
    heads = w_in.shape[2]
    head_dim = w_in.shape[3]
    projected = jnp.dot(x_ln, w_in.reshape(w_in.shape[0], -1), preferred_element_type=jnp.float32)
    projected = projected.astype(jnp.bfloat16).astype(jnp.float32).reshape(length, 4, heads, head_dim)
    logits = jnp.einsum('qhd,khd->hqk', projected[:, 0], projected[:, 1]) * head_dim ** -0.5
    if bias_hqk is not None:
        logits = logits + bias_hqk.astype(jnp.float32)
    logits = jnp.where(key_mask[None, None, :] > 0, logits, -1e9)
    attn_probs = jax.nn.softmax(logits, axis=-1).astype(jnp.bfloat16).astype(jnp.float32)
    attended = jnp.einsum('hqk,khd->qhd', attn_probs, projected[:, 2])
    gated = (attended * jax.nn.sigmoid(projected[:, 3])).astype(jnp.bfloat16)
    return jnp.dot(gated.reshape(length, heads * head_dim), w_out.reshape(heads * head_dim, -1), preferred_element_type=jnp.float32)


def row_attention(msa_act, bias_hqk, msa_mask, w_in, w_out):
    def one_seq(inputs):
        seq_act, seq_mask = inputs
        return add_residual(seq_act, attend_one(layer_norm(seq_act), w_in, w_out, bias_hqk, seq_mask))
    return lax.map(one_seq, (msa_act, msa_mask))


def column_attention(msa_act, msa_mask, w_in, w_out):
    def one_col(inputs):
        col_act, col_mask = inputs
        return add_residual(col_act, attend_one(layer_norm(col_act), w_in, w_out, None, col_mask))
    result = lax.map(one_col, (jnp.swapaxes(msa_act, 0, 1), msa_mask.T))
    return jnp.swapaxes(result, 0, 1)


def outer_mean(msa_act, pair_act, msa_mask, w_in, w_out):
    num_seq, num_res, width = msa_act.shape
    mask_f32 = msa_mask.astype(jnp.float32)
    projected = jnp.dot(layer_norm(msa_act).reshape(num_seq * num_res, width), w_in.reshape(width, -1), preferred_element_type=jnp.float32)
    projected = projected.reshape(num_seq, num_res, 2, -1) * mask_f32[:, :, None, None]
    projected = projected.astype(jnp.bfloat16).astype(jnp.float32)
    left = jnp.swapaxes(projected[:, :, 0], 0, 1)
    right = projected[:, :, 1]
    pair_norm = jnp.dot(mask_f32.T, mask_f32)
    w_flat = w_out.reshape(-1, w_out.shape[-1])
    def one_row(inputs):
        left_row, norm_row = inputs
        outer = jnp.einsum('sp,sjq->jpq', left_row, right).astype(jnp.bfloat16)
        update = jnp.dot(outer.reshape(num_res, -1), w_flat, preferred_element_type=jnp.float32)
        return update / (1e-3 + norm_row[:, None])
    return add_residual(pair_act, lax.map(one_row, (left, pair_norm)))


def triangle_start(pair_act, res_mask, w_bias, w_in, w_out):
    pair_ln = layer_norm(pair_act)
    bias_hqk = pair_bias(pair_ln, w_bias)
    def one_row(row_ln):
        return attend_one(row_ln, w_in, w_out, bias_hqk, res_mask)
    return add_residual(pair_act, lax.map(one_row, pair_ln))


def triangle_end(pair_act, res_mask, w_bias, w_in, w_out):
    flipped = triangle_start(jnp.swapaxes(pair_act, 0, 1), res_mask, w_bias, w_in, w_out)
    return jnp.swapaxes(flipped, 0, 1)


def reference(msa_act, pair_act, msa_mask, res_mask, w_row_bias, w_row_in, w_row_out, w_col_in, w_col_out, w_opm_in, w_opm_out, w_ts_bias, w_ts_in, w_ts_out, w_te_bias, w_te_in, w_te_out):
    bias_first = pair_bias(layer_norm(pair_act), w_row_bias[0])
    msa_act = row_attention(msa_act, bias_first, msa_mask, w_row_in[0], w_row_out[0])
    msa_act = column_attention(msa_act, msa_mask, w_col_in[0], w_col_out[0])
    pair_act = outer_mean(msa_act, pair_act, msa_mask, w_opm_in[0], w_opm_out[0])
    pair_act = triangle_start(pair_act, res_mask, w_ts_bias[0], w_ts_in[0], w_ts_out[0])
    pair_act = triangle_end(pair_act, res_mask, w_te_bias[0], w_te_in[0], w_te_out[0])
    bias_second = pair_bias(layer_norm(pair_act), w_row_bias[1])
    msa_act = column_attention(msa_act, msa_mask, w_col_in[1], w_col_out[1])
    pair_act = outer_mean(msa_act, pair_act, msa_mask, w_opm_in[1], w_opm_out[1])
    msa_act = row_attention(msa_act, bias_second, msa_mask, w_row_in[1], w_row_out[1])
    pair_act = triangle_end(pair_act, res_mask, w_te_bias[1], w_te_in[1], w_te_out[1])
    pair_act = triangle_start(pair_act, res_mask, w_ts_bias[1], w_ts_in[1], w_ts_out[1])
    return msa_act, pair_act
```

```python
import functools

import jax
import jax.numpy as jnp
from jax import lax
from jax.experimental import pallas as pl
from jax.experimental.pallas import tpu as pltpu
from jax.sharding import PartitionSpec as P

F32 = jnp.float32
BF16 = jnp.bfloat16
LOG2E = 1.4426950408889634
NEG = -1e9
N = 8
R, W, S = 64, 128, 256

PH_RB1, PH_M1, PH_C1, PH_SB1, PH_Z1, PH_EB1, PH_RB2, PH_C2, PH_M2, PH_EB2, PH_Z2, PH_SB2 = range(12)


def mm(a, b):
    return jnp.dot(a, b, preferred_element_type=F32)


def mm_nt(a, b):
    return lax.dot_general(a, b, (((1,), (1,)), ((), ())), preferred_element_type=F32)


def iota(shape, dim):
    return lax.broadcasted_iota(jnp.int32, shape, dim)


def ln(x):
    mu = jnp.mean(x, axis=0, keepdims=True)
    c = x - mu
    var = jnp.mean(c * c, axis=0, keepdims=True)
    return (c * lax.rsqrt(var + 1e-5)).astype(BF16)


def rnd(x):
    return x.astype(BF16).astype(F32)


def low_lanes(rows):
    return iota((rows, W), 1) < R


def softmax_keys(x):
    e = jnp.exp2(x - jnp.max(x, axis=-2, keepdims=True))
    return (e * (1.0 / jnp.sum(e, axis=-2, keepdims=True))).astype(BF16)


def attend_pair(proj, heads, dim, bias_ref, key_mask, hm_ref, rm_ref):
    hd = heads * dim
    q, k, v, g = (proj[n * hd:(n + 1) * hd] for n in range(4))
    lo = low_lanes(hd)
    qbd = jnp.concatenate([jnp.where(lo, q, 0.0), jnp.where(lo, 0.0, q)], axis=0).astype(BF16)
    kt = jnp.transpose(k)
    kp = jnp.concatenate([kt[0:R], kt[R:W]], axis=1).astype(BF16)
    lhs = jnp.concatenate([kp] * heads, axis=0) * hm_ref[...]
    s = mm(lhs, qbd)
    x = s * (dim ** -0.5 * LOG2E) + bias_ref[...]
    x = jnp.where(key_mask[None] > 0, x.reshape(heads, R, W), NEG * LOG2E)
    p = softmax_keys(x).reshape(heads * R, W)
    vr = pltpu.roll(v, R, 1)
    v2 = jnp.concatenate([jnp.where(lo, v, vr), jnp.where(lo, vr, v)], axis=0).astype(BF16)
    vm = jnp.concatenate([v2] * (heads // 2), axis=1) * rm_ref[...]
    o2 = mm(vm, p)
    o = jnp.where(lo, o2[0:hd], o2[hd:2 * hd])
    return (o * jax.nn.sigmoid(g)).astype(BF16)


def kernel(axis, m_ref, z_ref, mt_ref, r_ref, wrb, wri, wro, wci, wco, woi, woo, wsb, wsi, wso, web, wei, weo, mo_ref, zo_ref,
           maskb, mp, mloc, rn, rkey, hm_r, rm_r, hm_t, rm_t, wro_t, wco_t, wso_t, weo_t, wall, wf,
           rowf, sm1, rm1, m1, sm2, rm2, aloc, remf, rem, cg, xop, zst, zf, sz, rz, pb,
           bm_r1, bm_r2, br_r1, br_r2, bm_s1, bm_s2, bm_e1, bm_e2, br_s1, br_s2, br_e1, br_e2, bt_r, bt_t, pq, send, recv):
    me = lax.axis_index(axis)
    peers = [lax.rem(me + k, N) for k in range(N)]
    senders = [lax.rem(me + N - k, N) for k in range(N)]

    def copy(ph, k, src, dst):
        return pltpu.make_async_remote_copy(
            src_ref=src, dst_ref=dst, send_sem=send.at[ph, k], recv_sem=recv.at[ph, k],
            device_id={axis: peers[k]}, device_id_type=pl.DeviceIdType.MESH)

    started = []

    def exchange(ph, src_of, dst_ref):
        for k in range(1, N):
            c = copy(ph, k, src_of(peers[k]), dst_ref.at[me])
            c.start()
            started.append(c)
        dst_ref[me] = src_of(me)[...]

    def arrive(ph, like, dst_ref):
        for k in range(1, N):
            copy(ph, k, like, dst_ref.at[senders[k]]).wait_recv()

    barrier = pltpu.get_barrier_semaphore()
    for k in range(1, N):
        pl.semaphore_signal(barrier, inc=1, device_id={axis: peers[k]}, device_id_type=pl.DeviceIdType.MESH)

    def bias_message(xln, w_bias, heads, msg):
        half = heads // 2
        b = mm(w_bias, xln)
        if heads == 4:
            b = jnp.concatenate([b, b], axis=0)
        bh = pltpu.roll(b, 8 - half, 0)
        lo = low_lanes(8)
        for i in range(8):
            bl_v = b[:, W * (i // 2):W * (i // 2) + W]
            bh_v = bh[:, W * (i // 2):W * (i // 2) + W]
            if i % 2 == 0:
                pb[8 * i:8 * i + 8, :] = jnp.where(lo, bl_v, pltpu.roll(bh_v, R, 1))
            else:
                pb[8 * i:8 * i + 8, :] = jnp.where(lo, pltpu.roll(bl_v, R, 1), bh_v)
        msg[...] = jnp.concatenate([pb[pl.ds(h, 8, stride=8), :] for h in range(half)], axis=0).astype(BF16)

    def bias_table(got, heads, table, gathered_keys):
        half = heads // 2
        full = got[...].astype(F32) * LOG2E
        for h in range(half):
            x = full[:, 8 * h:8 * h + 8, :].reshape(R, W)
            if gathered_keys:
                xr = pltpu.roll(x, R, 1)
                lo = low_lanes(R)
                table[R * h:R * h + R, :] = jnp.where(lo, x, xr)
                table[R * (half + h):R * (half + h) + R, :] = jnp.where(lo, xr, x)
            else:
                t = jnp.transpose(x)
                for hp in range(2):
                    blk = t[R * hp:R * hp + R]
                    table[R * (half * hp + h):R * (half * hp + h) + R, :] = jnp.concatenate([blk, blk], axis=1)

    def z_features():
        return jnp.concatenate(
            [jnp.transpose(zst[W * t:W * t + W, :].astype(F32)) for t in range(4)], axis=1)

    zst[...] = z_ref[...].reshape(512, W)
    bias_message(ln(z_features()), wrb[0], 8, bm_r1)
    pl.semaphore_wait(barrier, N - 1)
    exchange(PH_RB1, lambda p: bm_r1, br_r1)

    mt = mt_ref[...].astype(F32)
    mt_b = mt.astype(BF16)
    sel = (iota((S, W), 0) == 32 * me + iota((S, W), 1)) & (iota((S, W), 1) < 32)
    mloc[...] = mm(mt_b, jnp.where(sel, 1.0, 0.0).astype(BF16)).astype(BF16)
    mrows = mt_ref[pl.ds(pl.multiple_of(8 * me, 8), 8), :].astype(F32)
    t = iota((S, S), 1)
    perm = iota((S, S), 0) == (t % W) // 16 * 32 + t // W * 16 + t % 16
    mperm = mm(mrows.astype(BF16), jnp.where(perm, 1.0, 0.0).astype(BF16))
    mp[...] = mperm
    mpt = jnp.transpose(mperm)
    for i in range(8):
        maskb[i] = jnp.broadcast_to(mpt[:, i:i + 1], (S, W))
        row = jnp.broadcast_to(mrows[i:i + 1, :], (W, S)).astype(BF16)
        rn[i] = 1.0 / (1e-3 + mm_nt(mt_b, row))
    rkey[...] = jnp.transpose(jnp.broadcast_to(r_ref[...].astype(F32), (W, R)))

    def fill(ref, fn):
        ref[...] = jnp.where(fn(iota(ref.shape, 0), iota(ref.shape, 1)), 1.0, 0.0).astype(BF16)

    fill(hm_r, lambda r, c: r // R == (c % R) // 8)
    fill(rm_r, lambda r, c: (r % R) // 8 == c // R)
    fill(hm_t, lambda r, c: r // R == (c % W) // 32)
    fill(rm_t, lambda r, c: (r % W) // 32 == c // R)
    for b in range(2):
        wro_t[b] = jnp.transpose(wro[b].astype(F32)).astype(BF16)
        wco_t[b] = jnp.transpose(wco[b].astype(F32)).astype(BF16)
        wso_t[b] = jnp.transpose(wso[b].astype(F32)).astype(BF16)
        weo_t[b] = jnp.transpose(weo[b].astype(F32)).astype(BF16)
    wf[...] = woo[0].astype(F32)
    for n in range(32):
        a, b = n // 4, n % 4
        wall[0, 32 * a:32 * a + 32, W * b:W * b + W] = wf[pl.ds(n, 32, stride=32), :].astype(BF16)
        wall[1, 32 * a:32 * a + 32, W * b:W * b + W] = woo[1, 32 * n:32 * n + 32, :]

    def row_attention(b, xt, pair):
        proj = rnd(mm(wri[b], ln(xt)))
        r, c = iota((W, W), 0), iota((W, W), 1)
        pick = r == jnp.where(c < R, pair, pair + 16)
        key_mask = mm(mloc[...], jnp.where(pick, 1.0, 0.0).astype(BF16))
        gated = attend_pair(proj, 8, 8, bt_r, key_mask, hm_r, rm_r)
        return rnd(xt + mm(wro_t[b], gated))

    arrive(PH_RB1, bm_r1, br_r1)
    bias_table(br_r1, 8, bt_r, False)

    def row1(pair, carry):
        x = jnp.concatenate([m_ref[pair], m_ref[pair + 16]], axis=0).astype(F32)
        y = row_attention(0, jnp.transpose(x), pair)
        yt = jnp.transpose(y)
        rowf[pl.ds(pl.multiple_of(R * pair, R), R), :] = jnp.concatenate([yt[0:R], yt[R:W]], axis=1)
        return carry

    lax.fori_loop(0, 16, row1, 0)
    for i in range(R):
        sm1[i // 8, i % 8] = rowf[pl.ds(i, 16, stride=R), :].astype(BF16)
    exchange(PH_M1, lambda p: sm1.at[p], rm1)

    def column_attention(b, xt, i):
        proj = rnd(mm(wci[b], ln(xt)))
        q, k, v, g = (proj[R * n:R * n + R] for n in range(4))
        kt = jnp.transpose(k).astype(BF16)
        head = iota((R, S), 0) // 8
        key_mask = maskb[i] > 0
        out = []
        for h in range(8):
            s = mm(kt, jnp.where(head == h, q, 0.0).astype(BF16))
            vh = v[8 * h:8 * h + 8].astype(BF16)
            parts = []
            for n in range(2):
                x = jnp.where(key_mask, s[:, W * n:W * n + W] * (8 ** -0.5 * LOG2E), NEG * LOG2E)
                parts.append(softmax_keys(x))
            out.append(mm(vh, jnp.concatenate(parts, axis=1)))
        o = jnp.concatenate(out, axis=0)
        gated = (o * jax.nn.sigmoid(g)).astype(BF16)
        return rnd(xt + mm(wco_t[b], gated))

    def opm_operands(b, xt, i):
        proj = mm(woi[b], ln(xt)) * mp[pl.ds(i, 1), :]
        near, far = (proj[0:32], proj[32:R]) if b == 0 else (proj[32:R], proj[0:32])
        rows = pl.ds(pl.multiple_of(32 * i, 32), 32)
        aloc[b, rows, :] = near.astype(BF16)
        remf[0, rows, :] = far[:, 0:W]
        remf[1, rows, :] = far[:, W:S]

    def pack_far(b):
        for n in range(16):
            for t in range(2):
                rem[b, 16 * n:16 * n + 16, W * t:W * t + W] = jnp.concatenate(
                    [remf[t, pl.ds(2 * n + u, 8, stride=32), :] for u in range(2)], axis=0).astype(BF16)

    arrive(PH_M1, sm1.at[0], rm1)

    def col1(i, carry):
        x = rm1[:, i].reshape(W, W).astype(F32)
        xt = jnp.transpose(x)
        y = column_attention(0, jnp.concatenate([xt[0:R], xt[R:W]], axis=1), i)
        m1[i] = y.astype(BF16)
        opm_operands(0, y, i)
        return carry

    lax.fori_loop(0, 8, col1, 0)
    pack_far(0)
    exchange(PH_C1, lambda p: rem.at[0], cg.at[0])

    def col2(i, carry):
        y = column_attention(1, m1[i].astype(F32), i)
        opm_operands(1, y, i)
        yt = jnp.transpose(jnp.concatenate([y[:, 0:W], y[:, W:S]], axis=0)).astype(BF16)
        sm2[:, i] = yt.reshape(8, 16, W)
        return carry

    lax.fori_loop(0, 8, col2, 0)
    exchange(PH_M2, lambda p: sm2.at[p], rm2)
    pack_far(1)

    def opm(b):
        for n in range(8):
            far = cg[b, :, 32 * n:32 * n + 32, :].reshape(S, S)
            o = mm_nt(aloc[b], far).astype(BF16)
            for i in range(8):
                xop[i, 32 * n:32 * n + 32, :] = o[32 * i:32 * i + 32, :]

        def one(i, carry):
            y = mm(jnp.transpose(xop[i]), wall[b]).reshape(8, 4, 8, 512)
            u = sum(y[:, n, :, W * n:W * n + W] for n in range(4)).reshape(R, W)
            rows = pl.ds(pl.multiple_of(R * i, R), R)
            zst[rows, :] = (zst[rows, :].astype(F32) + u * rn[i]).astype(BF16)
            return carry

        lax.fori_loop(0, 8, one, 0)

    def tri_project(xln, w_in):
        pq[...] = rnd(mm(w_in, xln))

    def tri_attend(x, w_out_t):
        out = []
        for t in range(4):
            gated = attend_pair(pq[:, W * t:W * t + W], 4, 32, bt_t, rkey[...], hm_t, rm_t)
            out.append(rnd(x[:, W * t:W * t + W] + mm(w_out_t, gated)))
        return jnp.concatenate(out, axis=1)

    def swap_pair(y, n):
        for t in range(4):
            zf[W * t:W * t + W, :] = jnp.transpose(y[:, W * t:W * t + W])
        for c in range(32):
            sz[n, 16 * c:16 * c + 16, :] = jnp.concatenate(
                [zf[pl.ds(2 * c, 8, stride=R), :], zf[pl.ds(2 * c + 1, 8, stride=R), :]], axis=0).astype(BF16)

    def take_pair(n):
        x = rz[n].astype(F32).reshape(8, 8, 8, W)
        for j in range(8):
            zst[R * j:R * j + R, :] = x[:, j].reshape(R, W).astype(BF16)

    def z_block(n, p):
        return sz.at[n, pl.ds(pl.multiple_of(R * p, R), R), :]

    arrive(PH_C1, rem.at[0], cg.at[0])
    exchange(PH_C2, lambda p: rem.at[1], cg.at[1])
    opm(0)
    x = z_features()
    xln = ln(x)
    bias_message(xln, wsb[0], 4, bm_s1)
    exchange(PH_SB1, lambda p: bm_s1, br_s1)
    tri_project(xln, wsi[0])
    arrive(PH_SB1, bm_s1, br_s1)
    bias_table(br_s1, 4, bt_t, False)
    y = tri_attend(x, wso_t[0])
    swap_pair(y, 0)
    exchange(PH_Z1, lambda p: z_block(0, p), rz.at[0])
    bias_message(ln(y), web[0], 4, bm_e1)
    exchange(PH_EB1, lambda p: bm_e1, br_e1)
    arrive(PH_Z1, z_block(0, 0), rz.at[0])
    take_pair(0)
    x = z_features()
    tri_project(ln(x), wei[0])
    arrive(PH_EB1, bm_e1, br_e1)
    bias_table(br_e1, 4, bt_t, True)
    y = tri_attend(x, weo_t[0])
    bias_message(ln(y), wrb[1], 8, bm_r2)
    exchange(PH_RB2, lambda p: bm_r2, br_r2)
    for t in range(4):
        zst[W * t:W * t + W, :] = jnp.transpose(y[:, W * t:W * t + W]).astype(BF16)

    arrive(PH_C2, rem.at[1], cg.at[1])
    opm(1)
    x = z_features()
    xln = ln(x)
    bias_message(xln, web[1], 4, bm_e2)
    exchange(PH_EB2, lambda p: bm_e2, br_e2)
    tri_project(xln, wei[1])

    arrive(PH_M2, sm2.at[0], rm2)
    arrive(PH_RB2, bm_r2, br_r2)
    bias_table(br_r2, 8, bt_r, True)
    rowf[...] = rm2[...].reshape(1024, W).astype(F32)

    def row2(pair, carry):
        xt = jnp.transpose(rowf[pl.ds(pair, R, stride=16), :])
        xm = jnp.concatenate([xt[0:R], xt[R:W]], axis=1)
        yt = jnp.transpose(row_attention(1, xm, pair)).astype(BF16)
        mo_ref[pair] = yt[0:R]
        mo_ref[pair + 16] = yt[R:W]
        return carry

    lax.fori_loop(0, 16, row2, 0)

    arrive(PH_EB2, bm_e2, br_e2)
    bias_table(br_e2, 4, bt_t, False)
    y = tri_attend(x, weo_t[1])
    swap_pair(y, 1)
    exchange(PH_Z2, lambda p: z_block(1, p), rz.at[1])
    bias_message(ln(y), wsb[1], 4, bm_s2)
    exchange(PH_SB2, lambda p: bm_s2, br_s2)
    arrive(PH_Z2, z_block(1, 0), rz.at[1])
    take_pair(1)
    x = z_features()
    tri_project(ln(x), wsi[1])
    arrive(PH_SB2, bm_s2, br_s2)
    bias_table(br_s2, 4, bt_t, True)
    y = tri_attend(x, wso_t[1])
    for t in range(4):
        zo_ref[2 * t:2 * t + 2] = jnp.transpose(y[:, W * t:W * t + W]).astype(BF16).reshape(2, R, W)

    for c in started:
        c.wait_send()


def solution(mesh):
    axis = 'dap'

    def local_step(m, z, msa_mask, res_mask, w_row_bias, w_row_in, w_row_out, w_col_in, w_col_out, w_opm_in, w_opm_out,
                   w_ts_bias, w_ts_in, w_ts_out, w_te_bias, w_te_in, w_te_out):
        def tin(w):
            return jnp.moveaxis(w, 1, -1).reshape(2, -1, w.shape[1])

        args = (m, z, msa_mask.T, res_mask[None, :],
                tin(w_row_bias), tin(w_row_in), w_row_out.reshape(2, R, R), tin(w_col_in), w_col_out.reshape(2, R, R),
                tin(w_opm_in), w_opm_out.reshape(2, 1024, W),
                tin(w_ts_bias), tin(w_ts_in), w_ts_out.reshape(2, W, W),
                tin(w_te_bias), tin(w_te_in), w_te_out.reshape(2, W, W))
        v = pltpu.VMEM
        scratch = [
            v((8, S, W), F32), v((8, S), F32), v((R, W), BF16), v((8, R, W), F32), v((R, W), F32),
            v((512, W), BF16), v((W, 512), BF16), v((S, S), BF16), v((S, S), BF16),
            v((2, R, R), BF16), v((2, R, R), BF16), v((2, W, W), BF16), v((2, W, W), BF16),
            v((2, S, 512), BF16), v((1024, W), F32),
            v((1024, W), F32), v((8, 8, 16, W), BF16), v((8, 8, 16, W), BF16), v((8, R, S), BF16),
            v((8, 8, 16, W), BF16), v((8, 8, 16, W), BF16),
            v((2, S, S), BF16), v((2, S, W), F32), v((2, S, S), BF16), v((2, 8, S, S), BF16), v((8, S, S), BF16),
            v((512, W), BF16), v((512, W), F32), v((2, 512, W), BF16), v((2, 8, R, W), BF16), v((R, W), F32),
            v((32, W), BF16), v((32, W), BF16), v((8, 32, W), BF16), v((8, 32, W), BF16),
            v((16, W), BF16), v((16, W), BF16), v((16, W), BF16), v((16, W), BF16),
            v((8, 16, W), BF16), v((8, 16, W), BF16), v((8, 16, W), BF16), v((8, 16, W), BF16),
            v((512, W), F32), v((S, W), F32), v((512, 512), F32),
            pltpu.SemaphoreType.DMA((12, N)), pltpu.SemaphoreType.DMA((12, N)),
        ]
        vmem = pl.BlockSpec(memory_space=pltpu.VMEM)
        return pl.pallas_call(
            functools.partial(kernel, axis),
            out_shape=(jax.ShapeDtypeStruct((32, R, R), BF16), jax.ShapeDtypeStruct((8, R, W), BF16)),
            in_specs=[vmem] * len(args),
            out_specs=(vmem, vmem),
            scratch_shapes=scratch,
            compiler_params=pltpu.CompilerParams(collective_id=0, has_side_effects=True, vmem_limit_bytes=58 * 1024 * 1024),
        )(*args)

    in_specs = (P(('data', 'dap')), P(('data', 'dap')), P('data'), P('data')) + (P(),) * 13
    out_specs = (P(('data', 'dap')), P(('data', 'dap')))
    return jax.shard_map(local_step, mesh=mesh, in_specs=in_specs, out_specs=out_specs, check_vma=False)
```

```python
import functools

import jax
import jax.numpy as jnp
from jax import lax
from jax.experimental import pallas as pl
from jax.experimental.pallas import tpu as pltpu
from jax.sharding import PartitionSpec as P

F32 = jnp.float32
BF16 = jnp.bfloat16
LOG2E = 1.4426950408889634
NEG = -1e9
NEG_PARTS = (-2835349504.0, 6914048.0, 8320.0)
N = 8
R, W, S, T, Q = 64, 128, 256, 512, 32

PH_RB1, PH_M1, PH_C1, PH_SB1, PH_Z1, PH_EB1, PH_RB2, PH_C2, PH_M2, PH_EB2, PH_Z2, PH_SB2 = range(12)


def mm(a, b):
    return jnp.dot(a, b, preferred_element_type=F32)


def mm_nt(a, b):
    return lax.dot_general(a, b, (((1,), (1,)), ((), ())), preferred_element_type=F32)


def iota(shape, dim):
    return lax.broadcasted_iota(jnp.int32, shape, dim)


def ln(x):
    mu = jnp.mean(x, axis=0, keepdims=True)
    c = x - mu
    var = jnp.mean(c * c, axis=0, keepdims=True)
    return (c * lax.rsqrt(var + 1e-5)).astype(BF16)


def rnd(x):
    return x.astype(BF16).astype(F32)


def low_lanes(rows):
    return iota((rows, W), 1) < R


def softmax_keys(x):
    e = jnp.exp2(x - jnp.max(x, axis=-2, keepdims=True))
    return (e * (1.0 / jnp.sum(e, axis=-2, keepdims=True))).astype(BF16)


def pair_logits(q, k, heads, hm_ref):
    lo = low_lanes(q.shape[0])
    qbd = jnp.concatenate([jnp.where(lo, q, 0.0), jnp.where(lo, 0.0, q)], axis=0).astype(BF16)
    kt = jnp.transpose(k)
    kp = jnp.concatenate([kt[0:R], kt[R:W]], axis=1).astype(BF16)
    return mm(jnp.concatenate([kp] * heads, axis=0) * hm_ref[...], qbd)


def pair_probs(s_ref, p_ref, heads, dim, bias_ref, key_mask):
    masked = key_mask > 0
    for h in range(heads):
        rows = slice(R * h, R * h + R)
        x = s_ref[rows, :] * (dim ** -0.5 * LOG2E) + bias_ref[rows, :]
        p_ref[rows, :] = softmax_keys(jnp.where(masked, x, NEG * LOG2E))


def pair_values(v, p_ref, heads, rm_ref):
    hd = v.shape[0]
    lo = low_lanes(hd)
    vr = pltpu.roll(v, R, 1)
    v2 = jnp.concatenate([jnp.where(lo, v, vr), jnp.where(lo, vr, v)], axis=0).astype(BF16)
    o2 = mm(jnp.concatenate([v2] * (heads // 2), axis=1) * rm_ref[...], p_ref[...])
    return jnp.where(lo, o2[0:hd], o2[hd:2 * hd])


def gate(o, g):
    return (o * jax.nn.sigmoid(g)).astype(BF16)


def kernel(axis, m_ref, z_ref, mt_ref, r_ref, wrb, wri, wro, wci, wco, woi, woo, wsb, wsi, wso, web, wei, weo, mo_ref, zo_ref,
           mp, mloc, rn, rkey, hm_r, rm_r, hm_t, rm_t, wro_t, wco_t, wso_t, weo_t, wall, wf,
           rowf, sm1, rm1, m1, sm2, rm2, aloc, remf, rem, cg, xop, zst, zf, sz, rz, pb,
           bm_r1, bm_r2, br_r1, br_r2, bm_s1, bm_s2, bm_e1, bm_e2, br_s1, br_s2, br_e1, br_e2, bt_r, bt_t, pq, sbuf, pbuf, pqm, xres, obuf, kaug, send, recv):
    me = lax.axis_index(axis)
    peers = [lax.rem(me + k, N) for k in range(N)]
    senders = [lax.rem(me + N - k, N) for k in range(N)]

    def copy(ph, k, src, dst):
        return pltpu.make_async_remote_copy(
            src_ref=src, dst_ref=dst, send_sem=send.at[ph, k], recv_sem=recv.at[ph, k],
            device_id={axis: peers[k]}, device_id_type=pl.DeviceIdType.MESH)

    started = []

    def exchange(ph, src_of, dst_ref):
        for k in range(1, N):
            c = copy(ph, k, src_of(peers[k]), dst_ref.at[me])
            c.start()
            started.append(c)
        dst_ref[me] = src_of(me)[...]

    def arrive(ph, like, dst_ref):
        for k in range(1, N):
            copy(ph, k, like, dst_ref.at[senders[k]]).wait_recv()

    barrier = pltpu.get_barrier_semaphore()
    for k in range(1, N):
        pl.semaphore_signal(barrier, inc=1, device_id={axis: peers[k]}, device_id_type=pl.DeviceIdType.MESH)

    def bias_message(xln, w_bias, heads, msg):
        half = heads // 2
        b = mm(w_bias, xln)
        if heads == 4:
            b = jnp.concatenate([b, b], axis=0)
        bh = pltpu.roll(b, 8 - half, 0)
        lo = low_lanes(8)
        for i in range(8):
            bl_v = b[:, W * (i // 2):W * (i // 2) + W]
            bh_v = bh[:, W * (i // 2):W * (i // 2) + W]
            if i % 2 == 0:
                pb[8 * i:8 * i + 8, :] = jnp.where(lo, bl_v, pltpu.roll(bh_v, R, 1))
            else:
                pb[8 * i:8 * i + 8, :] = jnp.where(lo, pltpu.roll(bl_v, R, 1), bh_v)
        msg[...] = jnp.concatenate([pb[pl.ds(h, 8, stride=8), :] for h in range(half)], axis=0).astype(BF16)

    def bias_table(got, heads, table, gathered_keys):
        half = heads // 2
        full = got[...].astype(F32) * LOG2E
        for h in range(half):
            x = full[:, 8 * h:8 * h + 8, :].reshape(R, W)
            if gathered_keys:
                xr = pltpu.roll(x, R, 1)
                lo = low_lanes(R)
                table[R * h:R * h + R, :] = jnp.where(lo, x, xr)
                table[R * (half + h):R * (half + h) + R, :] = jnp.where(lo, xr, x)
            else:
                t = jnp.transpose(x)
                for hp in range(2):
                    blk = t[R * hp:R * hp + R]
                    table[R * (half * hp + h):R * (half * hp + h) + R, :] = jnp.concatenate([blk, blk], axis=1)

    def z_features():
        return jnp.concatenate(
            [jnp.transpose(zst[W * t:W * t + W, :].astype(F32)) for t in range(4)], axis=1)

    zst[...] = z_ref[...].reshape(T, W)
    bias_message(ln(z_features()), wrb[0], 8, bm_r1)
    pl.semaphore_wait(barrier, N - 1)
    exchange(PH_RB1, lambda p: bm_r1, br_r1)

    mt = mt_ref[...].astype(F32)
    mt_b = mt.astype(BF16)
    sel = (iota((S, W), 0) == Q * me + iota((S, W), 1)) & (iota((S, W), 1) < Q)
    mloc[...] = mm(mt_b, jnp.where(sel, 1.0, 0.0).astype(BF16)).astype(BF16)
    mrows = mt_ref[pl.ds(pl.multiple_of(8 * me, 8), 8), :].astype(F32)
    t = iota((S, S), 1)
    perm = iota((S, S), 0) == (t % W) // 16 * Q + t // W * 16 + t % 16
    mperm = mm(mrows.astype(BF16), jnp.where(perm, 1.0, 0.0).astype(BF16))
    mp[...] = mperm
    for i in range(8):
        row = jnp.broadcast_to(mrows[i:i + 1, :], (W, S)).astype(BF16)
        rn[i] = 1.0 / (1e-3 + mm_nt(mt_b, row))
    rkey[...] = jnp.transpose(jnp.broadcast_to(r_ref[...].astype(F32), (W, R)))

    def fill(ref, fn):
        ref[...] = jnp.where(fn(iota(ref.shape, 0), iota(ref.shape, 1)), 1.0, 0.0).astype(BF16)

    fill(hm_r, lambda r, c: r // R == (c % R) // 8)
    fill(rm_r, lambda r, c: (r % R) // 8 == c // R)
    fill(hm_t, lambda r, c: r // R == (c % W) // Q)
    fill(rm_t, lambda r, c: (r % W) // Q == c // R)
    for b in range(2):
        wro_t[b] = jnp.transpose(wro[b].astype(F32)).astype(BF16)
        wco_t[b] = jnp.transpose(wco[b].astype(F32)).astype(BF16)
        wso_t[b] = jnp.transpose(wso[b].astype(F32)).astype(BF16)
        weo_t[b] = jnp.transpose(weo[b].astype(F32)).astype(BF16)
    wf[...] = woo[0].astype(F32)
    for n in range(Q):
        a, b = n // 4, n % 4
        wall[0, Q * a:Q * a + Q, W * b:W * b + W] = wf[pl.ds(n, Q, stride=Q), :].astype(BF16)
        wall[1, Q * a:Q * a + Q, W * b:W * b + W] = woo[1, Q * n:Q * n + Q, :]

    def row_attention(b, load, store):
        for c in range(4):
            x = jnp.concatenate([load(4 * c + t) for t in range(4)], axis=1)
            proj = rnd(mm(wri[b], ln(x)))
            for t in range(4):
                xres[4 * c + t] = x[:, W * t:W * t + W]
                pqm[4 * c + t] = proj[:, W * t:W * t + W]
        r, c = iota((W, W), 0), iota((W, W), 1)
        cs = jnp.where(c < R, 0, 16)

        def logits(pair, slot):
            sbuf[slot] = pair_logits(pqm[pair, 0:R, :], pqm[pair, R:2 * R, :], 8, hm_r)

        def probs(pair, slot):
            key_mask = mm(mloc[...], jnp.where(r == cs + pair, 1.0, 0.0).astype(BF16))
            pair_probs(sbuf.at[slot], pbuf.at[slot], 8, 8, bt_r, key_mask)

        def values(pair, slot):
            obuf[pair] = pair_values(pqm[pair, 2 * R:3 * R, :], pbuf.at[slot], 8, rm_r)

        return logits, probs, values

    def row_finish(b, store):
        for c in range(4):
            g = jnp.concatenate([pqm[4 * c + t, 3 * R:4 * R, :] for t in range(4)], axis=1)
            o = jnp.concatenate([obuf[4 * c + t] for t in range(4)], axis=1)
            x = jnp.concatenate([xres[4 * c + t] for t in range(4)], axis=1)
            y = rnd(x + mm(wro_t[b], gate(o, g)))
            for t in range(4):
                store(4 * c + t, jnp.transpose(y[:, W * t:W * t + W]))

    def row_stack(b, load, store):
        logits, probs, values = row_attention(b, load, store)
        logits(0, 0)

        def step(n, carry):
            logits(2 * n + 1, 1)
            probs(2 * n, 0)
            values(jnp.maximum(2 * n - 1, 0), 1)
            logits(jnp.minimum(2 * n + 2, 15), 0)
            probs(2 * n + 1, 1)
            values(2 * n, 0)
            return carry

        pbuf[1] = jnp.zeros((T, W), BF16)
        lax.fori_loop(0, 8, step, 0)
        values(15, 1)
        row_finish(b, store)

    arrive(PH_RB1, bm_r1, br_r1)
    bias_table(br_r1, 8, bt_r, False)

    def store1(pair, yt):
        rowf[R * pair:R * pair + R, :] = jnp.concatenate([yt[0:R], yt[R:W]], axis=1)

    row_stack(0, lambda pair: jnp.transpose(jnp.concatenate([m_ref[pair], m_ref[pair + 16]], axis=0).astype(F32)), store1)
    for i in range(R):
        sm1[i // 8, i % 8] = rowf[pl.ds(i, 16, stride=R), :].astype(BF16)
    exchange(PH_M1, lambda p: sm1.at[p], rm1)

    def both(ref, i, rows=slice(None)):
        return jnp.concatenate([ref[2 * i, rows, :], ref[2 * i + 1, rows, :]], axis=1)

    def put(ref, i, value):
        ref[2 * i] = value[:, 0:W]
        ref[2 * i + 1] = value[:, W:S]

    def column_project(b, load):
        part = iota((R, S), 0)
        flags = jnp.where(part == 0, NEG_PARTS[0], jnp.where(part == 1, NEG_PARTS[1], jnp.where(part == 2, NEG_PARTS[2], 0.0)))
        for i in range(8):
            x = load(i)
            proj = rnd(mm(wci[b], ln(x)))
            put(xres, i, x)
            put(pqm, i, proj)
            keep = mp[i:i + 1, :]
            ka = jnp.concatenate([proj[R:2 * R] * keep, flags * (1.0 - keep)], axis=0)
            kaug[i] = jnp.transpose(ka).astype(BF16)

    def column_stack(b, load, finish):
        column_project(b, load)
        head = iota((R, S), 0) // 8
        ones = jnp.where(iota((R, S), 0) < 3, 1.0, 0.0)

        def logits(i, h, slot):
            q = jnp.where(head == h, both(pqm, i, slice(0, R)), 0.0)
            s = mm(kaug[i], jnp.concatenate([q, ones], axis=0).astype(BF16))
            sbuf[slot, 0:S, :] = s[:, 0:W]
            sbuf[slot, S:2 * S, :] = s[:, W:S]

        def probs(slot):
            for n in range(2):
                rows = slice(S * n, S * n + S)
                pbuf[slot, rows, :] = softmax_keys(sbuf[slot, rows, :] * (8 ** -0.5 * LOG2E))

        def values(i, h, slot):
            rows = slice(2 * R + 8 * h, 2 * R + 8 * h + 8)
            vh = both(pqm, i, rows).astype(BF16)
            p = jnp.concatenate([pbuf[slot, 0:S, :], pbuf[slot, S:2 * S, :]], axis=1)
            o = mm(vh, p)
            obuf[2 * i, 8 * h:8 * h + 8, :] = o[:, 0:W]
            obuf[2 * i + 1, 8 * h:8 * h + 8, :] = o[:, W:S]

        pbuf[1] = jnp.zeros((T, W), BF16)
        logits(0, 0, 0)

        def step(i, carry):
            for h in range(8):
                if h < 7:
                    logits(i, h + 1, (h + 1) % 2)
                else:
                    logits(jnp.minimum(i + 1, 7), 0, 0)
                probs(h % 2)
                if h == 0:
                    values(jnp.maximum(i - 1, 0), 7, 1)
                else:
                    values(i, h - 1, (h - 1) % 2)
            return carry

        lax.fori_loop(0, 8, step, 0)
        values(7, 7, 1)
        for i in range(8):
            y = rnd(both(xres, i) + mm(wco_t[b], gate(both(obuf, i), both(pqm, i, slice(3 * R, 4 * R)))))
            finish(i, y)

    def opm_operands(b, xt, i):
        proj = mm(woi[b], ln(xt)) * mp[i:i + 1, :]
        near, far = (proj[0:Q], proj[Q:R]) if b == 0 else (proj[Q:R], proj[0:Q])
        rows = slice(Q * i, Q * i + Q)
        aloc[b, rows, :] = near.astype(BF16)
        remf[0, rows, :] = far[:, 0:W]
        remf[1, rows, :] = far[:, W:S]

    def pack_far(b):
        for n in range(16):
            for t in range(2):
                rem[b, 16 * n:16 * n + 16, W * t:W * t + W] = jnp.concatenate(
                    [remf[t, pl.ds(2 * n + u, 8, stride=Q), :] for u in range(2)], axis=0).astype(BF16)

    arrive(PH_M1, sm1.at[0], rm1)

    def load1(i):
        xt = jnp.transpose(rm1[:, i].reshape(W, W).astype(F32))
        return jnp.concatenate([xt[0:R], xt[R:W]], axis=1)

    def finish1(i, y):
        m1[i] = y.astype(BF16)
        opm_operands(0, y, i)

    column_stack(0, load1, finish1)
    pack_far(0)
    exchange(PH_C1, lambda p: rem.at[0], cg.at[0])

    def finish2(i, y):
        opm_operands(1, y, i)
        yt = jnp.transpose(jnp.concatenate([y[:, 0:W], y[:, W:S]], axis=0)).astype(BF16)
        sm2[:, i] = yt.reshape(8, 16, W)

    column_stack(1, lambda i: m1[i].astype(F32), finish2)
    exchange(PH_M2, lambda p: sm2.at[p], rm2)
    pack_far(1)

    def opm(b):
        for n in range(8):
            far = cg[b, :, Q * n:Q * n + Q, :].reshape(S, S)
            o = mm_nt(aloc[b], far).astype(BF16)
            for i in range(8):
                xop[i, Q * n:Q * n + Q, :] = o[Q * i:Q * i + Q, :]

        def one(i, carry):
            y = mm(jnp.transpose(xop[i]), wall[b]).reshape(8, 4, 8, T)
            u = sum(y[:, n, :, W * n:W * n + W] for n in range(4)).reshape(R, W)
            rows = pl.ds(pl.multiple_of(R * i, R), R)
            zst[rows, :] = (zst[rows, :].astype(F32) + u * rn[i]).astype(BF16)
            return carry

        lax.fori_loop(0, 8, one, 0)

    def tri_project(xln, w_in):
        pq[...] = rnd(mm(w_in, xln))

    def tri_attend(x, w_out_t):
        def part(n, t):
            return pq[W * n:W * n + W, W * t:W * t + W]

        for t in range(4):
            sbuf[t, 0:S, :] = pair_logits(part(0, t), part(1, t), 4, hm_t)
        for t in range(4):
            pair_probs(sbuf.at[t], pbuf.at[t], 4, Q, bt_t, rkey[...])
        o = jnp.concatenate([pair_values(part(2, t), pbuf.at[t, 0:S], 4, rm_t) for t in range(4)], axis=1)
        return rnd(x + mm(w_out_t, gate(o, pq[3 * W:4 * W, :])))

    def swap_pair(y, n):
        for t in range(4):
            zf[W * t:W * t + W, :] = jnp.transpose(y[:, W * t:W * t + W])
        for c in range(Q):
            sz[n, 16 * c:16 * c + 16, :] = jnp.concatenate(
                [zf[pl.ds(2 * c, 8, stride=R), :], zf[pl.ds(2 * c + 1, 8, stride=R), :]], axis=0).astype(BF16)

    def take_pair(n):
        x = rz[n].astype(F32).reshape(8, 8, 8, W)
        for j in range(8):
            zst[R * j:R * j + R, :] = x[:, j].reshape(R, W).astype(BF16)

    def z_block(n, p):
        return sz.at[n, pl.ds(pl.multiple_of(R * p, R), R), :]

    arrive(PH_C1, rem.at[0], cg.at[0])
    exchange(PH_C2, lambda p: rem.at[1], cg.at[1])
    opm(0)
    x = z_features()
    xln = ln(x)
    bias_message(xln, wsb[0], 4, bm_s1)
    exchange(PH_SB1, lambda p: bm_s1, br_s1)
    tri_project(xln, wsi[0])
    arrive(PH_SB1, bm_s1, br_s1)
    bias_table(br_s1, 4, bt_t, False)
    y = tri_attend(x, wso_t[0])
    swap_pair(y, 0)
    exchange(PH_Z1, lambda p: z_block(0, p), rz.at[0])
    bias_message(ln(y), web[0], 4, bm_e1)
    exchange(PH_EB1, lambda p: bm_e1, br_e1)
    arrive(PH_Z1, z_block(0, 0), rz.at[0])
    take_pair(0)
    x = z_features()
    tri_project(ln(x), wei[0])
    arrive(PH_EB1, bm_e1, br_e1)
    bias_table(br_e1, 4, bt_t, True)
    y = tri_attend(x, weo_t[0])
    bias_message(ln(y), wrb[1], 8, bm_r2)
    exchange(PH_RB2, lambda p: bm_r2, br_r2)
    for t in range(4):
        zst[W * t:W * t + W, :] = jnp.transpose(y[:, W * t:W * t + W]).astype(BF16)

    arrive(PH_C2, rem.at[1], cg.at[1])
    opm(1)
    x = z_features()
    xln = ln(x)
    bias_message(xln, web[1], 4, bm_e2)
    exchange(PH_EB2, lambda p: bm_e2, br_e2)
    tri_project(xln, wei[1])

    arrive(PH_M2, sm2.at[0], rm2)
    arrive(PH_RB2, bm_r2, br_r2)
    bias_table(br_r2, 8, bt_r, True)
    rowf[...] = rm2[...].reshape(1024, W).astype(F32)

    def load2(pair):
        xt = jnp.transpose(rowf[pl.ds(pair, R, stride=16), :])
        return jnp.concatenate([xt[0:R], xt[R:W]], axis=1)

    def store2(pair, yt):
        mo_ref[pair] = yt[0:R].astype(BF16)
        mo_ref[pair + 16] = yt[R:W].astype(BF16)

    row_stack(1, load2, store2)

    arrive(PH_EB2, bm_e2, br_e2)
    bias_table(br_e2, 4, bt_t, False)
    y = tri_attend(x, weo_t[1])
    swap_pair(y, 1)
    exchange(PH_Z2, lambda p: z_block(1, p), rz.at[1])
    bias_message(ln(y), wsb[1], 4, bm_s2)
    exchange(PH_SB2, lambda p: bm_s2, br_s2)
    arrive(PH_Z2, z_block(1, 0), rz.at[1])
    take_pair(1)
    x = z_features()
    tri_project(ln(x), wsi[1])
    arrive(PH_SB2, bm_s2, br_s2)
    bias_table(br_s2, 4, bt_t, True)
    y = tri_attend(x, wso_t[1])
    for t in range(4):
        zo_ref[2 * t:2 * t + 2] = jnp.transpose(y[:, W * t:W * t + W]).astype(BF16).reshape(2, R, W)

    for c in started:
        c.wait_send()


def solution(mesh):
    axis = 'dap'

    def local_step(m, z, msa_mask, res_mask, w_row_bias, w_row_in, w_row_out, w_col_in, w_col_out, w_opm_in, w_opm_out,
                   w_ts_bias, w_ts_in, w_ts_out, w_te_bias, w_te_in, w_te_out):
        def tin(w):
            return jnp.moveaxis(w, 1, -1).reshape(2, -1, w.shape[1])

        args = (m, z, msa_mask.T, res_mask[None, :],
                tin(w_row_bias), tin(w_row_in), w_row_out.reshape(2, R, R), tin(w_col_in), w_col_out.reshape(2, R, R),
                tin(w_opm_in), w_opm_out.reshape(2, 1024, W),
                tin(w_ts_bias), tin(w_ts_in), w_ts_out.reshape(2, W, W),
                tin(w_te_bias), tin(w_te_in), w_te_out.reshape(2, W, W))
        v = pltpu.VMEM
        scratch = [
            v((8, S), F32), v((R, W), BF16), v((8, R, W), F32), v((R, W), F32),
            v((T, W), BF16), v((W, T), BF16), v((S, S), BF16), v((S, S), BF16),
            v((2, R, R), BF16), v((2, R, R), BF16), v((2, W, W), BF16), v((2, W, W), BF16),
            v((2, S, T), BF16), v((1024, W), F32),
            v((1024, W), F32), v((8, 8, 16, W), BF16), v((8, 8, 16, W), BF16), v((8, R, S), BF16),
            v((8, 8, 16, W), BF16), v((8, 8, 16, W), BF16),
            v((2, S, S), BF16), v((2, S, W), F32), v((2, S, S), BF16), v((2, 8, S, S), BF16), v((8, S, S), BF16),
            v((T, W), BF16), v((T, W), F32), v((2, T, W), BF16), v((2, 8, R, W), BF16), v((R, W), F32),
            v((Q, W), BF16), v((Q, W), BF16), v((8, Q, W), BF16), v((8, Q, W), BF16),
            v((16, W), BF16), v((16, W), BF16), v((16, W), BF16), v((16, W), BF16),
            v((8, 16, W), BF16), v((8, 16, W), BF16), v((8, 16, W), BF16), v((8, 16, W), BF16),
            v((T, W), F32), v((S, W), F32), v((T, T), F32),
            v((4, T, W), F32), v((4, T, W), BF16), v((16, S, W), F32), v((16, R, W), F32), v((16, R, W), F32), v((8, S, W), BF16),
            pltpu.SemaphoreType.DMA((12, N)), pltpu.SemaphoreType.DMA((12, N)),
        ]
        vmem = pl.BlockSpec(memory_space=pltpu.VMEM)
        return pl.pallas_call(
            functools.partial(kernel, axis),
            out_shape=(jax.ShapeDtypeStruct((Q, R, R), BF16), jax.ShapeDtypeStruct((8, R, W), BF16)),
            in_specs=[vmem] * len(args),
            out_specs=(vmem, vmem),
            scratch_shapes=scratch,
            compiler_params=pltpu.CompilerParams(collective_id=0, has_side_effects=True, vmem_limit_bytes=58 * 1024 * 1024),
        )(*args)

    in_specs = (P(('data', 'dap')), P(('data', 'dap')), P('data'), P('data')) + (P(),) * 13
    out_specs = (P(('data', 'dap')), P(('data', 'dap')))
    return jax.shard_map(local_step, mesh=mesh, in_specs=in_specs, out_specs=out_specs, check_vma=False)
```

```python
import functools

import jax
import jax.numpy as jnp
from jax import lax
from jax.experimental import pallas as pl
from jax.experimental.pallas import tpu as pltpu
from jax.sharding import PartitionSpec as P

F32 = jnp.float32
BF16 = jnp.bfloat16
LOG2E = 1.4426950408889634
NEG = -1e9
NEG_PARTS = (-2835349504.0, 6914048.0, 8320.0)
N = 8
R, W, S, T, Q = 64, 128, 256, 512, 32

PH_RB1, PH_M1, PH_C1, PH_SB1, PH_Z1, PH_EB1, PH_RB2, PH_C2, PH_M2, PH_EB2, PH_Z2, PH_SB2 = range(12)


def mm(a, b):
    return jnp.dot(a, b, preferred_element_type=F32)


def mm_nt(a, b):
    return lax.dot_general(a, b, (((1,), (1,)), ((), ())), preferred_element_type=F32)


def iota(shape, dim):
    return lax.broadcasted_iota(jnp.int32, shape, dim)


def ln(x):
    mu = jnp.mean(x, axis=0, keepdims=True)
    c = x - mu
    var = jnp.mean(c * c, axis=0, keepdims=True)
    return (c * lax.rsqrt(var + 1e-5)).astype(BF16)


def rnd(x):
    return x.astype(BF16).astype(F32)


def low_lanes(rows):
    return iota((rows, W), 1) < R


def softmax_keys(x, scale):
    e = jnp.exp2((x - jnp.max(x, axis=-2, keepdims=True)) * scale)
    return (e * (1.0 / jnp.sum(e, axis=-2, keepdims=True))).astype(BF16)


def pair_logits(q, k, heads, hm_ref):
    lo = low_lanes(q.shape[0])
    qbd = jnp.concatenate([jnp.where(lo, q, 0.0), jnp.where(lo, 0.0, q)], axis=0).astype(BF16)
    kt = jnp.transpose(k)
    kp = jnp.concatenate([kt[0:R], kt[R:W]], axis=1).astype(BF16)
    return mm(jnp.concatenate([kp] * heads, axis=0) * hm_ref[...], qbd)


def pair_probs(s_ref, p_ref, heads, dim, bias_ref, key_mask):
    masked = key_mask > 0
    for h in range(heads):
        rows = slice(R * h, R * h + R)
        x = s_ref[rows, :] * dim ** -0.5 + bias_ref[rows, :]
        p_ref[rows, :] = softmax_keys(jnp.where(masked, x, NEG), LOG2E)


def pair_values(v, p_ref, heads, rm_ref):
    hd = v.shape[0]
    lo = low_lanes(hd)
    vr = pltpu.roll(v, R, 1)
    v2 = jnp.concatenate([jnp.where(lo, v, vr), jnp.where(lo, vr, v)], axis=0).astype(BF16)
    o2 = mm(jnp.concatenate([v2] * (heads // 2), axis=1) * rm_ref[...], p_ref[...])
    return jnp.where(lo, o2[0:hd], o2[hd:2 * hd])


def gate(o, g):
    return (o * jax.nn.sigmoid(g)).astype(BF16)


def kernel(axis, m_ref, z_ref, mt_ref, r_ref, wrb, wri, wro, wci, wco, woi, woo, wsb, wsi, wso, web, wei, weo, mo_ref, zo_ref,
           mp, mloc, rn, rkey, hm_r, rm_r, hm_t, rm_t, wro_t, wco_t, wso_t, weo_t, wall, wf,
           rowf, sm1, rm1, m1, sm2, rm2, aloc, remf, rem, cg, xop, zst, zf, sz, rz, pb,
           bm_r1, bm_r2, br_r1, br_r2, bm_s1, bm_s2, bm_e1, bm_e2, br_s1, br_s2, br_e1, br_e2, bt_r, bt_t, pq, sbuf, pbuf, pqm, xres, obuf, kaug, stri, ptri, send, recv):
    me = lax.axis_index(axis)
    peers = [lax.rem(me + k, N) for k in range(N)]
    senders = [lax.rem(me + N - k, N) for k in range(N)]

    def copy(ph, k, src, dst):
        return pltpu.make_async_remote_copy(
            src_ref=src, dst_ref=dst, send_sem=send.at[ph, k], recv_sem=recv.at[ph, k],
            device_id={axis: peers[k]}, device_id_type=pl.DeviceIdType.MESH)

    started = []

    chip, core = me // 2, lax.rem(me, 2)
    mate = me + 1 - 2 * core
    chip_x = chip + 1 - 2 * lax.rem(chip, 2)
    chips = [chip_x, lax.rem(chip + 2, 4), lax.rem(chip_x + 2, 4)]

    def send_to(ph, n, src, dst, device):
        return pltpu.make_async_remote_copy(
            src_ref=src, dst_ref=dst, send_sem=send.at[ph, n], recv_sem=recv.at[ph, n],
            device_id={axis: device}, device_id_type=pl.DeviceIdType.MESH)

    def far_copy(ph, b, n):
        to, slot = (2 * chips[n] + core, me) if n < 3 else (mate, me) if n == 3 else (mate, 2 * chips[n - 4] + core)
        return send_to(ph, n, rem.at[b] if n <= 3 else cg.at[b, slot], cg.at[b, slot], to)

    def far_start(ph, b, ns):
        for n in ns:
            far_copy(ph, b, n).start()
            started.append(functools.partial(far_copy, ph, b, n))

    def far_forward(ph, b):
        for n in range(3):
            send_to(ph, n, rem.at[b], cg.at[b, 2 * chips[n] + core], mate).wait_recv()
        far_start(ph, b, (4, 5, 6))

    def far_arrive(ph, b):
        send_to(ph, 3, rem.at[b], cg.at[b, mate], mate).wait_recv()
        for n in range(3):
            send_to(ph, 4 + n, rem.at[b], cg.at[b, 2 * chips[n] + 1 - core], mate).wait_recv()

    def exchange(ph, src_of, dst_ref):
        for k in range(1, N):
            c = functools.partial(copy, ph, k, src_of(peers[k]), dst_ref.at[me])
            c().start()
            started.append(c)
        dst_ref[me] = src_of(me)[...]

    def arrive(ph, like, dst_ref):
        for k in range(1, N):
            copy(ph, k, like, dst_ref.at[senders[k]]).wait_recv()

    barrier = pltpu.get_barrier_semaphore()
    for k in range(1, N):
        pl.semaphore_signal(barrier, inc=1, device_id={axis: peers[k]}, device_id_type=pl.DeviceIdType.MESH)

    def bias_message(xln, w_bias, heads, msg):
        half = heads // 2
        b = mm(w_bias, xln)
        if heads == 4:
            b = jnp.concatenate([b, b], axis=0)
        bh = pltpu.roll(b, N - half, 0)
        lo = low_lanes(N)
        for i in range(N):
            bl_v = b[:, W * (i // 2):W * (i // 2) + W]
            bh_v = bh[:, W * (i // 2):W * (i // 2) + W]
            if i % 2 == 0:
                pb[N * i:N * i + N, :] = jnp.where(lo, bl_v, pltpu.roll(bh_v, R, 1))
            else:
                pb[N * i:N * i + N, :] = jnp.where(lo, pltpu.roll(bl_v, R, 1), bh_v)
        msg[...] = jnp.concatenate([pb[pl.ds(h, N, stride=N), :] for h in range(half)], axis=0).astype(BF16)

    def bias_table(got, heads, table, gathered_keys):
        half = heads // 2
        full = got[...].astype(F32)
        for h in range(half):
            x = full[:, N * h:N * h + N, :].reshape(R, W)
            if gathered_keys:
                xr = pltpu.roll(x, R, 1)
                lo = low_lanes(R)
                table[R * h:R * h + R, :] = jnp.where(lo, x, xr)
                table[R * (half + h):R * (half + h) + R, :] = jnp.where(lo, xr, x)
            else:
                t = jnp.transpose(x)
                for hp in range(2):
                    blk = t[R * hp:R * hp + R]
                    table[R * (half * hp + h):R * (half * hp + h) + R, :] = jnp.concatenate([blk, blk], axis=1)

    def z_features():
        return jnp.concatenate(
            [jnp.transpose(zst[W * t:W * t + W, :].astype(F32)) for t in range(4)], axis=1)

    zst[...] = z_ref[...].reshape(T, W)
    bias_message(ln(z_features()), wrb[0], N, bm_r1)
    pl.semaphore_wait(barrier, N - 1)
    exchange(PH_RB1, lambda p: bm_r1, br_r1)

    def fill(ref, fn):
        ref[...] = jnp.where(fn(iota(ref.shape, 0), iota(ref.shape, 1)), 1.0, 0.0).astype(BF16)

    def row_constants():
        mt_b = mt_ref[...].astype(F32).astype(BF16)
        sel = (iota((S, W), 0) == Q * me + iota((S, W), 1)) & (iota((S, W), 1) < Q)
        mloc[...] = mm(mt_b, jnp.where(sel, 1.0, 0.0).astype(BF16)).astype(BF16)
        fill(hm_r, lambda r, c: r // R == (c % R) // N)
        fill(rm_r, lambda r, c: (r % R) // N == c // R)
        for b in range(2):
            wro_t[b] = jnp.transpose(wro[b].astype(F32)).astype(BF16)

    def other_constants():
        mt_b = mt_ref[...].astype(F32).astype(BF16)
        mrows = mt_ref[pl.ds(pl.multiple_of(N * me, N), N), :].astype(F32)
        t = iota((S, S), 1)
        perm = iota((S, S), 0) == (t % W) // 16 * Q + t // W * 16 + t % 16
        mp[...] = mm(mrows.astype(BF16), jnp.where(perm, 1.0, 0.0).astype(BF16))
        for i in range(N):
            row = jnp.broadcast_to(mrows[i:i + 1, :], (W, S)).astype(BF16)
            rn[i] = 1.0 / (1e-3 + mm_nt(mt_b, row))
        rkey[...] = jnp.transpose(jnp.broadcast_to(r_ref[...].astype(F32), (W, R)))
        fill(hm_t, lambda r, c: r // R == (c % W) // Q)
        fill(rm_t, lambda r, c: (r % W) // Q == c // R)
        for b in range(2):
            wco_t[b] = jnp.transpose(wco[b].astype(F32)).astype(BF16)
            wso_t[b] = jnp.transpose(wso[b].astype(F32)).astype(BF16)
            weo_t[b] = jnp.transpose(weo[b].astype(F32)).astype(BF16)
        wf[...] = woo[0].astype(F32)
        for n in range(Q):
            a, b = n // 4, n % 4
            wall[0, Q * a:Q * a + Q, W * b:W * b + W] = wf[pl.ds(n, Q, stride=Q), :].astype(BF16)
            wall[1, Q * a:Q * a + Q, W * b:W * b + W] = woo[1, Q * n:Q * n + Q, :]

    def row_project(b, load):
        for c in range(4):
            x = jnp.concatenate([load(4 * c + t) for t in range(4)], axis=1)
            proj = rnd(mm(wri[b], ln(x)))
            for t in range(4):
                xres[4 * c + t] = x[:, W * t:W * t + W]
                pqm[4 * c + t] = proj[:, W * t:W * t + W]

    def row_loop(lo, hi):
        r, c = iota((W, W), 0), iota((W, W), 1)
        cs = jnp.where(c < R, 0, 16)

        def logits(pair, slot):
            sbuf[slot] = pair_logits(pqm[pair, 0:R, :], pqm[pair, R:2 * R, :], N, hm_r)

        def probs(pair, slot):
            key_mask = mm(mloc[...], jnp.where(r == cs + pair, 1.0, 0.0).astype(BF16))
            pair_probs(sbuf.at[slot], pbuf.at[slot], N, N, bt_r, key_mask)

        def values(pair, slot):
            obuf[pair] = pair_values(pqm[pair, 2 * R:3 * R, :], pbuf.at[slot], N, rm_r)

        def step(n, carry):
            for t in range(4):
                p = 4 * n + t
                logits(jnp.minimum(p + 2, 15), (t + 2) % 4)
                probs(p, t)
                values(jnp.maximum(p - 1, 0), (t + 3) % 4)
            return carry

        if lo == 0:
            pbuf[3] = jnp.zeros((T, W), BF16)
            logits(0, 0)
            logits(1, 1)
        lax.fori_loop(lo, hi, step, 0)
        if hi == 4:
            values(15, 3)

    def row_finish(b, store):
        for c in range(4):
            g = jnp.concatenate([pqm[4 * c + t, 3 * R:4 * R, :] for t in range(4)], axis=1)
            o = jnp.concatenate([obuf[4 * c + t] for t in range(4)], axis=1)
            x = jnp.concatenate([xres[4 * c + t] for t in range(4)], axis=1)
            y = rnd(x + mm(wro_t[b], gate(o, g)))
            for t in range(4):
                store(4 * c + t, jnp.transpose(y[:, W * t:W * t + W]))

    row_constants()
    row_project(0, lambda pair: jnp.transpose(jnp.concatenate([m_ref[pair], m_ref[pair + 16]], axis=0).astype(F32)))
    arrive(PH_RB1, bm_r1, br_r1)
    bias_table(br_r1, N, bt_r, False)
    row_loop(0, 4)

    def store1(pair, yt):
        rowf[R * pair:R * pair + R, :] = jnp.concatenate([yt[0:R], yt[R:W]], axis=1)

    row_finish(0, store1)
    for i in range(R):
        sm1[i // N, i % N] = rowf[pl.ds(i, 16, stride=R), :].astype(BF16)
    exchange(PH_M1, lambda p: sm1.at[p], rm1)
    other_constants()

    def both(ref, i, rows=slice(None)):
        return jnp.concatenate([ref[2 * i, rows, :], ref[2 * i + 1, rows, :]], axis=1)

    def put(ref, i, value):
        ref[2 * i] = value[:, 0:W]
        ref[2 * i + 1] = value[:, W:S]

    def column_project(b, load):
        part = iota((R, S), 0)
        flags = jnp.where(part == 0, NEG_PARTS[0], jnp.where(part == 1, NEG_PARTS[1], jnp.where(part == 2, NEG_PARTS[2], 0.0)))
        for i in range(N):
            x = load(i)
            proj = rnd(mm(wci[b], ln(x)))
            put(xres, i, x)
            put(pqm, i, proj)
            keep = mp[i:i + 1, :]
            ka = jnp.concatenate([proj[R:2 * R] * keep, flags * (1.0 - keep)], axis=0)
            kaug[i] = jnp.transpose(ka).astype(BF16)

    def column_stack(b, load, finish, midway=None):
        column_project(b, load)
        head = iota((R, S), 0) // N
        ones = jnp.where(iota((R, S), 0) < 3, 1.0, 0.0)

        def logits(i, h, slot):
            q = jnp.where(head == h, both(pqm, i, slice(0, R)), 0.0)
            s = mm(kaug[i], jnp.concatenate([q, ones], axis=0).astype(BF16))
            sbuf[slot, 0:S, :] = s[:, 0:W]
            sbuf[slot, S:2 * S, :] = s[:, W:S]

        def probs(slot):
            for n in range(2):
                rows = slice(S * n, S * n + S)
                pbuf[slot, rows, :] = softmax_keys(sbuf[slot, rows, :], N ** -0.5 * LOG2E)

        def values(i, h, slot):
            rows = slice(2 * R + N * h, 2 * R + N * h + N)
            vh = both(pqm, i, rows).astype(BF16)
            p = jnp.concatenate([pbuf[slot, 0:S, :], pbuf[slot, S:2 * S, :]], axis=1)
            o = mm(vh, p)
            obuf[2 * i, N * h:N * h + N, :] = o[:, 0:W]
            obuf[2 * i + 1, N * h:N * h + N, :] = o[:, W:S]

        pbuf[3] = jnp.zeros((T, W), BF16)
        logits(0, 0, 0)
        logits(0, 1, 1)

        def step(i, carry):
            later = jnp.minimum(i + 1, 7)
            if midway is not None:
                pl.when(i == 6)(midway)
            for h in range(N):
                logits(i if h < 6 else later, (h + 2) % N, (h + 2) % 4)
                probs(h % 4)
                values(jnp.maximum(i - 1, 0) if h == 0 else i, (h + 7) % N, (h + 3) % 4)
            return carry

        lax.fori_loop(0, N, step, 0)
        values(7, 7, 3)
        for i in range(N):
            y = rnd(both(xres, i) + mm(wco_t[b], gate(both(obuf, i), both(pqm, i, slice(3 * R, 4 * R)))))
            finish(i, y)

    def opm_operands(b, xt, i):
        proj = mm(woi[b], ln(xt)) * mp[i:i + 1, :]
        near, far = (proj[0:Q], proj[Q:R]) if b == 0 else (proj[Q:R], proj[0:Q])
        rows = slice(Q * i, Q * i + Q)
        aloc[b, rows, :] = near.astype(BF16)
        remf[0, rows, :] = far[:, 0:W]
        remf[1, rows, :] = far[:, W:S]

    def pack_far(b):
        for n in range(16):
            for t in range(2):
                rem[b, 16 * n:16 * n + 16, W * t:W * t + W] = jnp.concatenate(
                    [remf[t, pl.ds(2 * n + u, N, stride=Q), :] for u in range(2)], axis=0).astype(BF16)

    arrive(PH_M1, sm1.at[0], rm1)

    def load1(i):
        xt = jnp.transpose(rm1[:, i].reshape(W, W).astype(F32))
        return jnp.concatenate([xt[0:R], xt[R:W]], axis=1)

    def finish1(i, y):
        m1[i] = y.astype(BF16)
        opm_operands(0, y, i)

    column_stack(0, load1, finish1)
    pack_far(0)
    far_start(PH_C1, 0, (0, 1, 2, 3))
    cg[0, me] = rem[0]

    def finish2(i, y):
        opm_operands(1, y, i)
        yt = jnp.transpose(jnp.concatenate([y[:, 0:W], y[:, W:S]], axis=0)).astype(BF16)
        sm2[:, i] = yt.reshape(N, 16, W)

    column_stack(1, lambda i: m1[i].astype(F32), finish2, lambda: far_forward(PH_C1, 0))
    pack_far(1)

    def opm(b):
        for n in range(N):
            far = cg[b, :, Q * n:Q * n + Q, :].reshape(S, S)
            o = mm_nt(aloc[b], far).astype(BF16)
            for i in range(N):
                xop[i, Q * n:Q * n + Q, :] = o[Q * i:Q * i + Q, :]

        for i in range(N):
            y = mm(jnp.transpose(xop[i]), wall[b]).reshape(N, 4, N, T)
            u = sum(y[:, n, :, W * n:W * n + W] for n in range(4)).reshape(R, W)
            rows = slice(R * i, R * i + R)
            zst[rows, :] = (zst[rows, :].astype(F32) + u * rn[i]).astype(BF16)

    def tri_project(xln, w_in):
        pq[...] = rnd(mm(w_in, xln))

    def tri_attend(x, w_out_t):
        def part(n, t):
            return pq[W * n:W * n + W, W * t:W * t + W]

        for t in range(4):
            stri[t] = pair_logits(part(0, t), part(1, t), 4, hm_t)
        for t in range(4):
            pair_probs(stri.at[t], ptri.at[t], 4, Q, bt_t, rkey[...])
        o = jnp.concatenate([pair_values(part(2, t), ptri.at[t], 4, rm_t) for t in range(4)], axis=1)
        return rnd(x + mm(w_out_t, gate(o, pq[3 * W:4 * W, :])))

    def swap_pair(y, n):
        for t in range(4):
            zf[W * t:W * t + W, :] = jnp.transpose(y[:, W * t:W * t + W])
        for c in range(Q):
            sz[n, 16 * c:16 * c + 16, :] = jnp.concatenate(
                [zf[pl.ds(2 * c, N, stride=R), :], zf[pl.ds(2 * c + 1, N, stride=R), :]], axis=0).astype(BF16)

    def take_pair(n):
        x = rz[n].astype(F32).reshape(N, N, N, W)
        for j in range(N):
            zst[R * j:R * j + R, :] = x[:, j].reshape(R, W).astype(BF16)

    def z_block(n, p):
        return sz.at[n, pl.ds(pl.multiple_of(R * p, R), R), :]

    far_arrive(PH_C1, 0)
    far_start(PH_C2, 1, (0, 1, 3))
    cg[1, me] = rem[1]
    opm(0)
    x = z_features()
    xln = ln(x)
    bias_message(xln, wsb[0], 4, bm_s1)
    exchange(PH_SB1, lambda p: bm_s1, br_s1)
    far_start(PH_C2, 1, (2,))
    tri_project(xln, wsi[0])
    arrive(PH_SB1, bm_s1, br_s1)
    bias_table(br_s1, 4, bt_t, False)
    y = tri_attend(x, wso_t[0])
    swap_pair(y, 0)
    exchange(PH_Z1, lambda p: z_block(0, p), rz.at[0])
    bias_message(ln(y), web[0], 4, bm_e1)
    exchange(PH_EB1, lambda p: bm_e1, br_e1)
    far_forward(PH_C2, 1)
    exchange(PH_M2, lambda p: sm2.at[p], rm2)
    arrive(PH_Z1, z_block(0, 0), rz.at[0])
    take_pair(0)
    x = z_features()
    tri_project(ln(x), wei[0])
    arrive(PH_EB1, bm_e1, br_e1)
    bias_table(br_e1, 4, bt_t, True)
    y = tri_attend(x, weo_t[0])
    bias_message(ln(y), wrb[1], N, bm_r2)
    exchange(PH_RB2, lambda p: bm_r2, br_r2)
    for t in range(4):
        zst[W * t:W * t + W, :] = jnp.transpose(y[:, W * t:W * t + W]).astype(BF16)

    far_arrive(PH_C2, 1)
    opm(1)
    x = z_features()
    xln = ln(x)
    bias_message(xln, web[1], 4, bm_e2)
    exchange(PH_EB2, lambda p: bm_e2, br_e2)
    tri_project(xln, wei[1])

    arrive(PH_M2, sm2.at[0], rm2)
    rowf[...] = rm2[...].reshape(1024, W).astype(F32)

    def load2(pair):
        xt = jnp.transpose(rowf[pl.ds(pair, R, stride=16), :])
        return jnp.concatenate([xt[0:R], xt[R:W]], axis=1)

    def store2(pair, yt):
        mo_ref[pair] = yt[0:R].astype(BF16)
        mo_ref[pair + 16] = yt[R:W].astype(BF16)

    row_project(1, load2)
    arrive(PH_RB2, bm_r2, br_r2)
    bias_table(br_r2, N, bt_r, True)
    row_loop(0, 2)

    arrive(PH_EB2, bm_e2, br_e2)
    bias_table(br_e2, 4, bt_t, False)
    y = tri_attend(x, weo_t[1])
    swap_pair(y, 1)
    exchange(PH_Z2, lambda p: z_block(1, p), rz.at[1])
    bias_message(ln(y), wsb[1], 4, bm_s2)
    exchange(PH_SB2, lambda p: bm_s2, br_s2)
    row_loop(2, 4)
    row_finish(1, store2)
    arrive(PH_Z2, z_block(1, 0), rz.at[1])
    take_pair(1)
    x = z_features()
    tri_project(ln(x), wsi[1])
    arrive(PH_SB2, bm_s2, br_s2)
    bias_table(br_s2, 4, bt_t, True)
    y = tri_attend(x, wso_t[1])
    for t in range(4):
        zo_ref[2 * t:2 * t + 2] = jnp.transpose(y[:, W * t:W * t + W]).astype(BF16).reshape(2, R, W)

    for c in started:
        c().wait_send()


def solution(mesh):
    axis = 'dap'

    def local_step(m, z, msa_mask, res_mask, w_row_bias, w_row_in, w_row_out, w_col_in, w_col_out, w_opm_in, w_opm_out,
                   w_ts_bias, w_ts_in, w_ts_out, w_te_bias, w_te_in, w_te_out):
        def tin(w):
            return jnp.moveaxis(w, 1, -1).reshape(2, -1, w.shape[1])

        args = (m, z, msa_mask.T, res_mask[None, :],
                tin(w_row_bias), tin(w_row_in), w_row_out.reshape(2, R, R), tin(w_col_in), w_col_out.reshape(2, R, R),
                tin(w_opm_in), w_opm_out.reshape(2, 1024, W),
                tin(w_ts_bias), tin(w_ts_in), w_ts_out.reshape(2, W, W),
                tin(w_te_bias), tin(w_te_in), w_te_out.reshape(2, W, W))
        v = pltpu.VMEM
        scratch = [
            v((N, S), F32), v((R, W), BF16), v((N, R, W), F32), v((R, W), F32),
            v((T, W), BF16), v((W, T), BF16), v((S, S), BF16), v((S, S), BF16),
            v((2, R, R), BF16), v((2, R, R), BF16), v((2, W, W), BF16), v((2, W, W), BF16),
            v((2, S, T), BF16), v((1024, W), F32),
            v((1024, W), F32), v((N, N, 16, W), BF16), v((N, N, 16, W), BF16), v((N, R, S), BF16),
            v((N, N, 16, W), BF16), v((N, N, 16, W), BF16),
            v((2, S, S), BF16), v((2, S, W), F32), v((2, S, S), BF16), v((2, N, S, S), BF16), v((N, S, S), BF16),
            v((T, W), BF16), v((T, W), F32), v((2, T, W), BF16), v((2, N, R, W), BF16), v((R, W), F32),
            v((Q, W), BF16), v((Q, W), BF16), v((N, Q, W), BF16), v((N, Q, W), BF16),
            v((16, W), BF16), v((16, W), BF16), v((16, W), BF16), v((16, W), BF16),
            v((N, 16, W), BF16), v((N, 16, W), BF16), v((N, 16, W), BF16), v((N, 16, W), BF16),
            v((T, W), F32), v((S, W), F32), v((T, T), F32),
            v((4, T, W), F32), v((4, T, W), BF16), v((16, S, W), F32), v((16, R, W), F32), v((16, R, W), F32), v((N, S, W), BF16), v((4, S, W), F32), v((4, S, W), BF16),
            pltpu.SemaphoreType.DMA((12, N)), pltpu.SemaphoreType.DMA((12, N)),
        ]
        vmem = pl.BlockSpec(memory_space=pltpu.VMEM)
        return pl.pallas_call(
            functools.partial(kernel, axis),
            out_shape=(jax.ShapeDtypeStruct((Q, R, R), BF16), jax.ShapeDtypeStruct((N, R, W), BF16)),
            in_specs=[vmem] * len(args),
            out_specs=(vmem, vmem),
            scratch_shapes=scratch,
            compiler_params=pltpu.CompilerParams(collective_id=0, has_side_effects=True, vmem_limit_bytes=58 * 1024 * 1024),
        )(*args)

    in_specs = (P(('data', 'dap')), P(('data', 'dap')), P('data'), P('data')) + (P(),) * 13
    out_specs = (P(('data', 'dap')), P(('data', 'dap')))
    return jax.shard_map(local_step, mesh=mesh, in_specs=in_specs, out_specs=out_specs, check_vma=False)
```

```python
import functools

import jax
import jax.numpy as jnp
from jax import lax
from jax.experimental import pallas as pl
from jax.experimental.pallas import tpu as pltpu
from jax.sharding import PartitionSpec as P

F32 = jnp.float32
BF16 = jnp.bfloat16
LOG2E = 1.4426950408889634
NEG = -1e9
NEG_PARTS = (-2835349504.0, 6914048.0, 8320.0)
N = 8
R, W, S, T, Q = 64, 128, 256, 512, 32

PH_RB1, PH_M1, PH_SB1, PH_Z1, PH_EB1, PH_RB2, PH_M2, PH_EB2, PH_Z2, PH_SB2, PH_C = range(11)


def mm(a, b):
    return jnp.dot(a, b, preferred_element_type=F32)


def mm_nt(a, b):
    return lax.dot_general(a, b, (((1,), (1,)), ((), ())), preferred_element_type=F32)


def iota(shape, dim):
    return lax.broadcasted_iota(jnp.int32, shape, dim)


def ln(x):
    mu = jnp.mean(x, axis=0, keepdims=True)
    c = x - mu
    var = jnp.mean(c * c, axis=0, keepdims=True)
    return (c * lax.rsqrt(var + 1e-5)).astype(BF16)


def rnd(x):
    return x.astype(BF16).astype(F32)


def low_lanes(rows):
    return iota((rows, W), 1) < R


def softmax_keys(x, scale):
    e = jnp.exp2((x - jnp.max(x, axis=-2, keepdims=True)) * scale)
    return (e * (1.0 / jnp.sum(e, axis=-2, keepdims=True))).astype(BF16)


def pair_logits(q, k, heads, hm_ref):
    lo = low_lanes(q.shape[0])
    qbd = jnp.concatenate([jnp.where(lo, q, 0.0), jnp.where(lo, 0.0, q)], axis=0).astype(BF16)
    kt = jnp.transpose(k)
    kp = jnp.concatenate([kt[0:R], kt[R:W]], axis=1).astype(BF16)
    return mm(jnp.concatenate([kp] * heads, axis=0) * hm_ref[...], qbd)


def pair_probs(s_ref, p_ref, heads, dim, bias_ref, key_mask):
    masked = key_mask > 0
    for h in range(heads):
        rows = slice(R * h, R * h + R)
        x = s_ref[rows, :] * dim ** -0.5 + bias_ref[rows, :]
        p_ref[rows, :] = softmax_keys(jnp.where(masked, x, NEG), LOG2E)


def pair_values(v, p_ref, heads, rm_ref):
    hd = v.shape[0]
    lo = low_lanes(hd)
    vr = pltpu.roll(v, R, 1)
    v2 = jnp.concatenate([jnp.where(lo, v, vr), jnp.where(lo, vr, v)], axis=0).astype(BF16)
    o2 = mm(jnp.concatenate([v2] * (heads // 2), axis=1) * rm_ref[...], p_ref[...])
    return jnp.where(lo, o2[0:hd], o2[hd:2 * hd])


def gate(o, g):
    return (o * jax.nn.sigmoid(g)).astype(BF16)


def kernel(axis, *refs):
    hbm, refs = refs[:17], refs[17:]
    (mo_ref, zo_ref), held, (load_sem, *refs) = refs[:2], refs[2:19], refs[19:]
    m_ref, z_ref, mt_ref, r_ref, wrb, wri, wro, wci, wco, woi, woo, wsb, wsi, wso, web, wei, weo = held
    (mp, mloc, rn, rkey, hm_r, rm_r, hm_t, rm_t, wro_t, wco_t, wso_t, weo_t, wall, wf,
     rowf, sm1, rm1, m1, sm2, rm2, aloc, remf, rem, cg, xop, zst, zf, sz, rz, pb,
     bm_r1, bm_r2, br_r1, br_r2, bm_s1, bm_s2, bm_e1, bm_e2, br_s1, br_s2, br_e1, br_e2,
     bt_r, bt_t, pq, sbuf, pbuf, pqm, xres, obuf, kaug, stri, ptri, send, recv) = refs
    me = lax.axis_index(axis)
    peers = [lax.rem(me + k, N) for k in range(N)]
    senders = [lax.rem(me + N - k, N) for k in range(N)]

    def copy(ph, k, src, dst):
        return pltpu.make_async_remote_copy(
            src_ref=src, dst_ref=dst, send_sem=send.at[ph, k], recv_sem=recv.at[ph, k],
            device_id={axis: peers[k]}, device_id_type=pl.DeviceIdType.MESH)

    started = []
    loads = {id(held[n]): pltpu.make_async_copy(hbm[n], held[n], load_sem.at[n]) for n in range(17)}
    for ref in (z_ref, wrb, m_ref, mt_ref, wri, wro, r_ref, wci, wco, woi, woo, wsb, wsi, wso, web, wei, weo):
        loads[id(ref)].start()

    def need(*wanted):
        for ref in wanted:
            loads[id(ref)].wait()

    chip, core = me // 2, lax.rem(me, 2)
    mate = me + 1 - 2 * core
    chip_x = chip + 1 - 2 * lax.rem(chip, 2)
    chips = [chip_x, lax.rem(chip + 2, 4), lax.rem(chip_x + 2, 4)]

    def send_to(ph, n, src, dst, device):
        return pltpu.make_async_remote_copy(
            src_ref=src, dst_ref=dst, send_sem=send.at[ph, n], recv_sem=recv.at[ph, n],
            device_id={axis: device}, device_id_type=pl.DeviceIdType.MESH)

    def far_ref(ref, half):
        return ref.at[pl.ds(W * half, W), :]

    def far_copy(b, half, n):
        ph = PH_C + 2 * b + half
        if n <= 3:
            to = 2 * chips[n] + core if n < 3 else mate
            return send_to(ph, n, far_ref(rem.at[b], half), far_ref(cg.at[b, me], half), to)
        slot = far_ref(cg.at[b, 2 * chips[n - 4] + core], half)
        return send_to(ph, n, slot, slot, mate)

    def far_start(b, half, ns):
        for n in ns:
            far_copy(b, half, n).start()
            started.append(functools.partial(far_copy, b, half, n))

    def far_got(b, half, n, device):
        send_to(PH_C + 2 * b + half, n, far_ref(rem.at[b], half), far_ref(cg.at[b, device], half), mate).wait_recv()

    def far_forward(b, half, ns):
        for n in ns:
            far_got(b, half, n, 2 * chips[n] + core)
            far_start(b, half, (4 + n,))

    def far_arrive(b, half):
        far_got(b, half, 3, mate)
        for n in range(3):
            far_got(b, half, 4 + n, 2 * chips[n] + 1 - core)

    def exchange(ph, src_of, dst_ref):
        for k in range(1, N):
            c = functools.partial(copy, ph, k, src_of(peers[k]), dst_ref.at[me])
            c().start()
            started.append(c)
        dst_ref[me] = src_of(me)[...]

    def arrive(ph, like, dst_ref):
        for k in range(1, N):
            copy(ph, k, like, dst_ref.at[senders[k]]).wait_recv()

    barrier = pltpu.get_barrier_semaphore()
    for k in range(1, N):
        pl.semaphore_signal(barrier, inc=1, device_id={axis: peers[k]}, device_id_type=pl.DeviceIdType.MESH)

    def bias_message(xln, w_bias, heads, msg):
        half = heads // 2
        b = mm(w_bias, xln)
        if heads == 4:
            b = jnp.concatenate([b, b], axis=0)
        bh = pltpu.roll(b, N - half, 0)
        lo = low_lanes(N)
        for i in range(N):
            bl_v = b[:, W * (i // 2):W * (i // 2) + W]
            bh_v = bh[:, W * (i // 2):W * (i // 2) + W]
            if i % 2 == 0:
                pb[N * i:N * i + N, :] = jnp.where(lo, bl_v, pltpu.roll(bh_v, R, 1))
            else:
                pb[N * i:N * i + N, :] = jnp.where(lo, pltpu.roll(bl_v, R, 1), bh_v)
        msg[...] = jnp.concatenate([pb[pl.ds(h, N, stride=N), :] for h in range(half)], axis=0).astype(BF16)

    def bias_table(got, heads, table, gathered_keys):
        half = heads // 2
        full = got[...].astype(F32)
        for h in range(half):
            x = full[:, N * h:N * h + N, :].reshape(R, W)
            if gathered_keys:
                xr = pltpu.roll(x, R, 1)
                lo = low_lanes(R)
                table[R * h:R * h + R, :] = jnp.where(lo, x, xr)
                table[R * (half + h):R * (half + h) + R, :] = jnp.where(lo, xr, x)
            else:
                t = jnp.transpose(x)
                for hp in range(2):
                    blk = t[R * hp:R * hp + R]
                    table[R * (half * hp + h):R * (half * hp + h) + R, :] = jnp.concatenate([blk, blk], axis=1)

    def z_features():
        return jnp.concatenate(
            [jnp.transpose(zst[W * t:W * t + W, :].astype(F32)) for t in range(4)], axis=1)

    need(z_ref, wrb)
    zst[...] = z_ref[...].reshape(T, W)
    bias_message(ln(z_features()), wrb[0], N, bm_r1)
    pl.semaphore_wait(barrier, N - 1)
    exchange(PH_RB1, lambda p: bm_r1, br_r1)

    def fill(ref, fn):
        ref[...] = jnp.where(fn(iota(ref.shape, 0), iota(ref.shape, 1)), 1.0, 0.0).astype(BF16)

    def row_constants():
        mt_b = mt_ref[...].astype(F32).astype(BF16)
        sel = (iota((S, W), 0) == Q * me + iota((S, W), 1)) & (iota((S, W), 1) < Q)
        mloc[...] = mm(mt_b, jnp.where(sel, 1.0, 0.0).astype(BF16)).astype(BF16)
        fill(hm_r, lambda r, c: r // R == (c % R) // N)
        fill(rm_r, lambda r, c: (r % R) // N == c // R)
        for b in range(2):
            wro_t[b] = jnp.transpose(wro[b].astype(F32)).astype(BF16)

    def other_constants():
        mt_b = mt_ref[...].astype(F32).astype(BF16)
        mrows = mt_ref[pl.ds(pl.multiple_of(N * me, N), N), :].astype(F32)
        t = iota((S, S), 1)
        perm = iota((S, S), 0) == (t % W) // 16 * Q + t // W * 16 + t % 16
        mp[...] = mm(mrows.astype(BF16), jnp.where(perm, 1.0, 0.0).astype(BF16))
        for i in range(N):
            row = jnp.broadcast_to(mrows[i:i + 1, :], (W, S)).astype(BF16)
            rn[i] = 1.0 / (1e-3 + mm_nt(mt_b, row))
        rkey[...] = jnp.transpose(jnp.broadcast_to(r_ref[...].astype(F32), (W, R)))
        fill(hm_t, lambda r, c: r // R == (c % W) // Q)
        fill(rm_t, lambda r, c: (r % W) // Q == c // R)
        for b in range(2):
            wco_t[b] = jnp.transpose(wco[b].astype(F32)).astype(BF16)
            wso_t[b] = jnp.transpose(wso[b].astype(F32)).astype(BF16)
            weo_t[b] = jnp.transpose(weo[b].astype(F32)).astype(BF16)
        wf[...] = woo[0].astype(F32)
        for n in range(Q):
            a, b = n // 4, n % 4
            wall[0, Q * a:Q * a + Q, W * b:W * b + W] = wf[pl.ds(n, Q, stride=Q), :].astype(BF16)

    def row_project(b, load):
        for c in range(4):
            x = jnp.concatenate([load(4 * c + t) for t in range(4)], axis=1)
            proj = rnd(mm(wri[b], ln(x)))
            for t in range(4):
                xres[4 * c + t] = x[:, W * t:W * t + W]
                pqm[4 * c + t] = proj[:, W * t:W * t + W]

    def row_loop(lo, hi):
        r, c = iota((W, W), 0), iota((W, W), 1)
        cs = jnp.where(c < R, 0, 16)

        def logits(pair, slot):
            sbuf[slot] = pair_logits(pqm[pair, 0:R, :], pqm[pair, R:2 * R, :], N, hm_r)

        def probs(pair, slot):
            key_mask = mm(mloc[...], jnp.where(r == cs + pair, 1.0, 0.0).astype(BF16))
            pair_probs(sbuf.at[slot], pbuf.at[slot], N, N, bt_r, key_mask)

        def values(pair, slot):
            obuf[pair] = pair_values(pqm[pair, 2 * R:3 * R, :], pbuf.at[slot], N, rm_r)

        def step(n, carry):
            for t in range(4):
                p = 4 * n + t
                logits(jnp.minimum(p + 2, 15), (t + 2) % 4)
                probs(p, t)
                values(jnp.maximum(p - 1, 0), (t + 3) % 4)
            return carry

        if lo == 0:
            pbuf[3] = jnp.zeros((T, W), BF16)
            logits(0, 0)
            logits(1, 1)
        lax.fori_loop(lo, hi, step, 0)
        if hi == 4:
            values(15, 3)

    def row_finish(b, store):
        for c in range(4):
            g = jnp.concatenate([pqm[4 * c + t, 3 * R:4 * R, :] for t in range(4)], axis=1)
            o = jnp.concatenate([obuf[4 * c + t] for t in range(4)], axis=1)
            x = jnp.concatenate([xres[4 * c + t] for t in range(4)], axis=1)
            y = rnd(x + mm(wro_t[b], gate(o, g)))
            for t in range(4):
                store(4 * c + t, jnp.transpose(y[:, W * t:W * t + W]))

    need(m_ref, mt_ref, wri, wro)
    row_constants()
    row_project(0, lambda pair: jnp.transpose(jnp.concatenate([m_ref[pair], m_ref[pair + 16]], axis=0).astype(F32)))
    arrive(PH_RB1, bm_r1, br_r1)
    bias_table(br_r1, N, bt_r, False)
    row_loop(0, 4)

    def store1(pair, yt):
        rowf[R * pair:R * pair + R, :] = jnp.concatenate([yt[0:R], yt[R:W]], axis=1)

    row_finish(0, store1)
    for i in range(R):
        sm1[i // N, i % N] = rowf[pl.ds(i, 16, stride=R), :].astype(BF16)
    exchange(PH_M1, lambda p: sm1.at[p], rm1)
    need(r_ref, wci, wco, woi, woo, wsb, wsi, wso, web, wei, weo)
    other_constants()

    def both(ref, i, rows=slice(None)):
        return jnp.concatenate([ref[2 * i, rows, :], ref[2 * i + 1, rows, :]], axis=1)

    def put(ref, i, value):
        ref[2 * i] = value[:, 0:W]
        ref[2 * i + 1] = value[:, W:S]

    def column_project(b, load):
        part = iota((R, S), 0)
        flags = jnp.where(part == 0, NEG_PARTS[0], jnp.where(part == 1, NEG_PARTS[1], jnp.where(part == 2, NEG_PARTS[2], 0.0)))
        for i in range(N):
            x = load(i)
            proj = rnd(mm(wci[b], ln(x)))
            put(xres, i, x)
            put(pqm, i, proj)
            keep = mp[i:i + 1, :]
            ka = jnp.concatenate([proj[R:2 * R] * keep, flags * (1.0 - keep)], axis=0)
            kaug[i] = jnp.transpose(ka).astype(BF16)

    def column_stack(b, load, finish, midway=None):
        column_project(b, load)
        head = iota((R, S), 0) // N
        ones = jnp.where(iota((R, S), 0) < 3, 1.0, 0.0)

        def logits(i, h, slot):
            q = jnp.where(head == h, both(pqm, i, slice(0, R)), 0.0)
            s = mm(kaug[i], jnp.concatenate([q, ones], axis=0).astype(BF16))
            sbuf[slot, 0:S, :] = s[:, 0:W]
            sbuf[slot, S:2 * S, :] = s[:, W:S]

        def probs(slot):
            for n in range(2):
                rows = slice(S * n, S * n + S)
                pbuf[slot, rows, :] = softmax_keys(sbuf[slot, rows, :], N ** -0.5 * LOG2E)

        def values(i, h, slot):
            rows = slice(2 * R + N * h, 2 * R + N * h + N)
            vh = both(pqm, i, rows).astype(BF16)
            p = jnp.concatenate([pbuf[slot, 0:S, :], pbuf[slot, S:2 * S, :]], axis=1)
            o = mm(vh, p)
            obuf[2 * i, N * h:N * h + N, :] = o[:, 0:W]
            obuf[2 * i + 1, N * h:N * h + N, :] = o[:, W:S]

        pbuf[3] = jnp.zeros((T, W), BF16)
        logits(0, 0, 0)
        logits(0, 1, 1)

        def step(i, carry):
            later = jnp.minimum(i + 1, 7)
            if midway is not None:
                for half in range(2):
                    pl.when(i == (4, 7)[half])(functools.partial(midway, half))
            for h in range(N):
                logits(i if h < 6 else later, (h + 2) % N, (h + 2) % 4)
                probs(h % 4)
                values(jnp.maximum(i - 1, 0) if h == 0 else i, (h + 7) % N, (h + 3) % 4)
            return carry

        lax.fori_loop(0, N, step, 0)
        values(7, 7, 3)
        for i in range(N):
            y = rnd(both(xres, i) + mm(wco_t[b], gate(both(obuf, i), both(pqm, i, slice(3 * R, 4 * R)))))
            finish(i, y)

    def opm_operands(b, xt, i):
        proj = mm(woi[b], ln(xt)) * mp[i:i + 1, :]
        near, far = (proj[0:Q], proj[Q:R]) if b == 0 else (proj[Q:R], proj[0:Q])
        rows = slice(Q * i, Q * i + Q)
        aloc[b, rows, :] = near.astype(BF16)
        remf[0, rows, :] = far[:, 0:W]
        remf[1, rows, :] = far[:, W:S]

    def pack_far(b):
        for n in range(16):
            for t in range(2):
                rem[b, 16 * n:16 * n + 16, W * t:W * t + W] = jnp.concatenate(
                    [remf[t, pl.ds(2 * n + u, N, stride=Q), :] for u in range(2)], axis=0).astype(BF16)

    arrive(PH_M1, sm1.at[0], rm1)

    def load1(i):
        xt = jnp.transpose(rm1[:, i].reshape(W, W).astype(F32))
        return jnp.concatenate([xt[0:R], xt[R:W]], axis=1)

    def finish1(i, y):
        m1[i] = y.astype(BF16)
        opm_operands(0, y, i)

    column_stack(0, load1, finish1)
    pack_far(0)
    for half in range(2):
        far_start(0, half, (0, 1, 2, 3))
    cg[0, me] = rem[0]

    def finish2(i, y):
        opm_operands(1, y, i)
        yt = jnp.transpose(jnp.concatenate([y[:, 0:W], y[:, W:S]], axis=0)).astype(BF16)
        sm2[:, i] = yt.reshape(N, 16, W)

    column_stack(1, lambda i: m1[i].astype(F32), finish2, lambda half: far_forward(0, half, range(3)))
    pack_far(1)

    def opm(b):
        for n in range(N):
            if n % 4 == 0:
                far_arrive(b, n // 4)
            far = cg[b, :, Q * n:Q * n + Q, :].reshape(S, S)
            o = mm_nt(aloc[b], far).astype(BF16)
            for i in range(N):
                xop[i, Q * n:Q * n + Q, :] = o[Q * i:Q * i + Q, :]

        for i in range(N):
            y = mm(jnp.transpose(xop[i]), wall[b]).reshape(N, 4, N, T)
            u = sum(y[:, n, :, W * n:W * n + W] for n in range(4)).reshape(R, W)
            rows = slice(R * i, R * i + R)
            zst[rows, :] = (zst[rows, :].astype(F32) + u * rn[i]).astype(BF16)

    def tri_part(n, t):
        return pq[W * n:W * n + W, W * t:W * t + W]

    def tri_logits(xln, w_in):
        pq[...] = rnd(mm(w_in, xln))
        for t in range(4):
            stri[t] = pair_logits(tri_part(0, t), tri_part(1, t), 4, hm_t)

    def tri_attend(x, w_out_t):
        for t in range(4):
            pair_probs(stri.at[t], ptri.at[t], 4, Q, bt_t, rkey[...])
        o = jnp.concatenate([pair_values(tri_part(2, t), ptri.at[t], 4, rm_t) for t in range(4)], axis=1)
        return rnd(x + mm(w_out_t, gate(o, pq[3 * W:4 * W, :])))

    def swap_pair(y, n):
        for t in range(4):
            zf[W * t:W * t + W, :] = jnp.transpose(y[:, W * t:W * t + W])
        for c in range(Q):
            sz[n, 16 * c:16 * c + 16, :] = jnp.concatenate(
                [zf[pl.ds(2 * c, N, stride=R), :], zf[pl.ds(2 * c + 1, N, stride=R), :]], axis=0).astype(BF16)

    def take_pair(n):
        x = rz[n].astype(F32).reshape(N, N, N, W)
        for j in range(N):
            zst[R * j:R * j + R, :] = x[:, j].reshape(R, W).astype(BF16)

    def z_block(n, p):
        return sz.at[n, pl.ds(pl.multiple_of(R * p, R), R), :]

    far_start(1, 0, (0, 1, 3))
    cg[1, me] = rem[1]
    opm(0)
    x = z_features()
    xln = ln(x)
    bias_message(xln, wsb[0], 4, bm_s1)
    exchange(PH_SB1, lambda p: bm_s1, br_s1)
    far_start(1, 0, (2,))
    far_start(1, 1, (0, 1, 3))
    tri_logits(xln, wsi[0])
    arrive(PH_SB1, bm_s1, br_s1)
    bias_table(br_s1, 4, bt_t, False)
    y = tri_attend(x, wso_t[0])
    swap_pair(y, 0)
    exchange(PH_Z1, lambda p: z_block(0, p), rz.at[0])
    bias_message(ln(y), web[0], 4, bm_e1)
    exchange(PH_EB1, lambda p: bm_e1, br_e1)
    far_start(1, 1, (2,))
    exchange(PH_M2, lambda p: sm2.at[p], rm2)
    far_forward(1, 0, range(3))
    far_forward(1, 1, range(2))
    for n in range(Q):
        wall[1, Q * (n // 4):Q * (n // 4) + Q, W * (n % 4):W * (n % 4) + W] = woo[1, Q * n:Q * n + Q, :]
    arrive(PH_Z1, z_block(0, 0), rz.at[0])
    take_pair(0)
    x = z_features()
    tri_logits(ln(x), wei[0])
    arrive(PH_EB1, bm_e1, br_e1)
    bias_table(br_e1, 4, bt_t, True)
    y = tri_attend(x, weo_t[0])
    far_forward(1, 1, (2,))
    bias_message(ln(y), wrb[1], N, bm_r2)
    exchange(PH_RB2, lambda p: bm_r2, br_r2)
    for t in range(4):
        zst[W * t:W * t + W, :] = jnp.transpose(y[:, W * t:W * t + W]).astype(BF16)

    opm(1)
    x = z_features()
    xln = ln(x)
    bias_message(xln, web[1], 4, bm_e2)
    exchange(PH_EB2, lambda p: bm_e2, br_e2)
    tri_logits(xln, wei[1])

    arrive(PH_M2, sm2.at[0], rm2)
    rowf[...] = rm2[...].reshape(1024, W).astype(F32)

    def load2(pair):
        xt = jnp.transpose(rowf[pl.ds(pair, R, stride=16), :])
        return jnp.concatenate([xt[0:R], xt[R:W]], axis=1)

    def store2(pair, yt):
        mo_ref[pair] = yt[0:R]
        mo_ref[pair + 16] = yt[R:W]

    row_project(1, load2)
    arrive(PH_RB2, bm_r2, br_r2)
    bias_table(br_r2, N, bt_r, True)
    row_loop(0, 2)

    arrive(PH_EB2, bm_e2, br_e2)
    bias_table(br_e2, 4, bt_t, False)
    y = tri_attend(x, weo_t[1])
    swap_pair(y, 1)
    exchange(PH_Z2, lambda p: z_block(1, p), rz.at[1])
    bias_message(ln(y), wsb[1], 4, bm_s2)
    exchange(PH_SB2, lambda p: bm_s2, br_s2)
    row_loop(2, 4)
    row_finish(1, store2)
    arrive(PH_Z2, z_block(1, 0), rz.at[1])
    take_pair(1)
    x = z_features()
    tri_logits(ln(x), wsi[1])
    arrive(PH_SB2, bm_s2, br_s2)
    bias_table(br_s2, 4, bt_t, True)
    y = tri_attend(x, wso_t[1])
    for t in range(4):
        zo_ref[2 * t:2 * t + 2] = jnp.transpose(y[:, W * t:W * t + W]).reshape(2, R, W)

    for c in started:
        c().wait_send()


def solution(mesh):
    axis = 'dap'

    def local_step(m, z, msa_mask, res_mask, w_row_bias, w_row_in, w_row_out, w_col_in, w_col_out, w_opm_in, w_opm_out,
                   w_ts_bias, w_ts_in, w_ts_out, w_te_bias, w_te_in, w_te_out):
        def tin(w):
            return jnp.moveaxis(w, 1, -1).reshape(2, -1, w.shape[1])

        args = (m, z, msa_mask.T, res_mask[None, :],
                tin(w_row_bias), tin(w_row_in), w_row_out.reshape(2, R, R), tin(w_col_in), w_col_out.reshape(2, R, R),
                tin(w_opm_in), w_opm_out.reshape(2, 1024, W),
                tin(w_ts_bias), tin(w_ts_in), w_ts_out.reshape(2, W, W),
                tin(w_te_bias), tin(w_te_in), w_te_out.reshape(2, W, W))
        v = pltpu.VMEM
        scratch = [v(a.shape, a.dtype) for a in args] + [
            pltpu.SemaphoreType.DMA((17,)),
            v((N, S), F32), v((R, W), BF16), v((N, R, W), F32), v((R, W), F32),
            v((T, W), BF16), v((W, T), BF16), v((S, S), BF16), v((S, S), BF16),
            v((2, R, R), BF16), v((2, R, R), BF16), v((2, W, W), BF16), v((2, W, W), BF16),
            v((2, S, T), BF16), v((1024, W), F32),
            v((1024, W), F32), v((N, N, 16, W), BF16), v((N, N, 16, W), BF16), v((N, R, S), BF16),
            v((N, N, 16, W), BF16), v((N, N, 16, W), BF16),
            v((2, S, S), BF16), v((2, S, W), F32), v((2, S, S), BF16), v((2, N, S, S), BF16), v((N, S, S), BF16),
            v((T, W), BF16), v((T, W), F32), v((2, T, W), BF16), v((2, N, R, W), BF16), v((R, W), F32),
            v((Q, W), BF16), v((Q, W), BF16), v((N, Q, W), BF16), v((N, Q, W), BF16),
            v((16, W), BF16), v((16, W), BF16), v((16, W), BF16), v((16, W), BF16),
            v((N, 16, W), BF16), v((N, 16, W), BF16), v((N, 16, W), BF16), v((N, 16, W), BF16),
            v((T, W), F32), v((S, W), F32), v((T, T), F32),
            v((4, T, W), F32), v((4, T, W), BF16), v((16, S, W), F32), v((16, R, W), F32), v((16, R, W), F32), v((N, S, W), BF16), v((4, S, W), F32), v((4, S, W), BF16),
            pltpu.SemaphoreType.DMA((15, N)), pltpu.SemaphoreType.DMA((15, N)),
        ]
        vmem = pl.BlockSpec(memory_space=pltpu.VMEM)
        mo, zo = pl.pallas_call(
            functools.partial(kernel, axis),
            out_shape=(jax.ShapeDtypeStruct((Q, R, R), F32), jax.ShapeDtypeStruct((N, R, W), F32)),
            in_specs=[pl.BlockSpec(memory_space=pltpu.HBM)] * len(args),
            out_specs=(vmem, vmem),
            scratch_shapes=scratch,
            compiler_params=pltpu.CompilerParams(collective_id=0, has_side_effects=True, vmem_limit_bytes=60 * 1024 * 1024),
        )(*args)
        return mo.astype(BF16), zo.astype(BF16)

    in_specs = (P(('data', 'dap')), P(('data', 'dap')), P('data'), P('data')) + (P(),) * 13
    out_specs = (P(('data', 'dap')), P(('data', 'dap')))
    return jax.shard_map(local_step, mesh=mesh, in_specs=in_specs, out_specs=out_specs, check_vma=False)
```

```python
import functools

import jax
import jax.numpy as jnp
from jax import lax
from jax.experimental import pallas as pl
from jax.experimental.pallas import tpu as pltpu
from jax.sharding import PartitionSpec as P

F32 = jnp.float32
BF16 = jnp.bfloat16
LOG2E = 1.4426950408889634
NEG = -1e9
NEG_PARTS = (-2835349504.0, 6914048.0, 8320.0)
N = 8
R, W, S, T, Q, H = 64, 128, 256, 512, 32, 16
TWO, FOUR = range(2), range(4)

PH_RB1, PH_SB1, PH_Z1, PH_EB1, PH_RB2, PH_M2, PH_EB2, PH_Z2, PH_SB2, PH_M1, PH_M1B, PH_C = range(12)


def mm(a, b):
    return jnp.dot(a, b, preferred_element_type=F32)


def mm_nt(a, b):
    return lax.dot_general(a, b, (((1,), (1,)), ((), ())), preferred_element_type=F32)


def iota(shape, dim):
    return lax.broadcasted_iota(jnp.int32, shape, dim)


def ln(x):
    mu = jnp.mean(x, axis=0, keepdims=True)
    c = x - mu
    var = jnp.mean(c * c, axis=0, keepdims=True)
    return (c * lax.rsqrt(var + 1e-5)).astype(BF16)


def rnd(x):
    return x.astype(BF16).astype(F32)


def flag(x):
    return jnp.where(x, 1.0, 0.0)


def low_lanes(rows):
    return iota((rows, W), 1) < R


def softmax_keys(x, scale):
    e = jnp.exp2((x - jnp.max(x, axis=-2, keepdims=True)) * scale)
    return (e * (1.0 / jnp.sum(e, axis=-2, keepdims=True))).astype(BF16)


def pair_logits(q, k, heads, hm_ref):
    lo = low_lanes(q.shape[0])
    qbd = jnp.concatenate([jnp.where(lo, q, 0.0), jnp.where(lo, 0.0, q)], axis=0).astype(BF16)
    kt = jnp.transpose(k)
    kp = jnp.concatenate([kt[0:R], kt[R:W]], axis=1).astype(BF16)
    return mm(jnp.concatenate([kp] * heads, axis=0) * hm_ref[...], qbd)


def pair_probs(s_ref, p_ref, heads, dim, bias_ref, key_mask):
    masked = key_mask > 0
    for h in range(heads):
        rows = slice(R * h, R * h + R)
        x = s_ref[rows, :] * dim ** -0.5 + bias_ref[rows, :]
        p_ref[rows, :] = softmax_keys(jnp.where(masked, x, NEG), LOG2E)


def pair_values(v, p_ref, heads, rm_ref):
    hd = v.shape[0]
    lo = low_lanes(hd)
    vr = pltpu.roll(v, R, 1)
    v2 = jnp.concatenate([jnp.where(lo, v, vr), jnp.where(lo, vr, v)], axis=0).astype(BF16)
    o2 = mm(jnp.concatenate([v2] * (heads // 2), axis=1) * rm_ref[...], p_ref[...])
    return jnp.where(lo, o2[0:hd], o2[hd:2 * hd])


def gate(o, g):
    return (o * jax.nn.sigmoid(g)).astype(BF16)


def kernel(axis, *refs):
    hbm, refs = refs[:17], refs[17:]
    (mo_ref, zo_ref), held, (load_sem, *refs) = refs[:2], refs[2:19], refs[19:]
    m_ref, z_ref, mt_ref, r_ref, wrb, wri, wro, wci, wco, woi, woo, wsb, wsi, wso, web, wei, weo = held
    (mp, mloc, rn, rkey, hm_r, rm_r, hm_t, rm_t, wro_t, wco_t, wso_t, weo_t, wall, wf,
     rowf, sm1, rm1, m1, sm2, rm2, aloc, remf, rem, cg, xop, zst, zf, sz, rz, pb,
     bm_r1, bm_r2, br_r1, br_r2, bm_s1, bm_s2, bm_e1, bm_e2, br_s1, br_s2, br_e1, br_e2,
     bt_r, bt_t, pq, sbuf, pbuf, pqm, xres, obuf, kaug, stri, ptri, mst, send, recv) = refs
    me = lax.axis_index(axis)
    peers = [lax.rem(me + k, N) for k in range(N)]
    senders = [lax.rem(me + N - k, N) for k in range(N)]

    def copy(ph, k, src, dst):
        return pltpu.make_async_remote_copy(
            src_ref=src, dst_ref=dst, send_sem=send.at[ph, k], recv_sem=recv.at[ph, k],
            device_id={axis: peers[k]}, device_id_type=pl.DeviceIdType.MESH)

    started = []
    loads = {id(held[n]): pltpu.make_async_copy(hbm[n], held[n], load_sem.at[n]) for n in range(17)}
    for ref in (z_ref, wrb, m_ref, mt_ref, wri, wro, r_ref, wci, wco, woi, woo, wsb, wsi, wso, web, wei, weo):
        loads[id(ref)].start()

    def need(*wanted):
        for ref in wanted:
            loads[id(ref)].wait()

    chip, core = me // 2, lax.rem(me, 2)
    mate = me + 1 - 2 * core
    chip_x = chip + 1 - 2 * lax.rem(chip, 2)
    chips = [chip_x, lax.rem(chip + 2, 4), lax.rem(chip_x + 2, 4)]

    def send_to(ph, n, src, dst, device):
        return pltpu.make_async_remote_copy(
            src_ref=src, dst_ref=dst, send_sem=send.at[ph, n], recv_sem=recv.at[ph, n],
            device_id={axis: device}, device_id_type=pl.DeviceIdType.MESH)

    def far_ref(ref, half):
        return ref.at[pl.ds(W * half, W), :]

    def far_copy(b, half, n):
        ph = PH_C + 2 * b + half
        if n <= 3:
            to = 2 * chips[n] + core if n < 3 else mate
            return send_to(ph, n, far_ref(rem.at[b], half), far_ref(cg.at[b, me], half), to)
        slot = far_ref(cg.at[b, 2 * chips[n - 4] + core], half)
        return send_to(ph, n, slot, slot, mate)

    def far_start(b, half, ns):
        for n in ns:
            far_copy(b, half, n).start()
            started.append(functools.partial(far_copy, b, half, n))

    def far_got(b, half, n, device):
        send_to(PH_C + 2 * b + half, n, far_ref(rem.at[b], half), far_ref(cg.at[b, device], half), mate).wait_recv()

    def far_forward(b, half, ns):
        for n in ns:
            far_got(b, half, n, 2 * chips[n] + core)
            far_start(b, half, (4 + n,))

    def far_arrive(b, half):
        far_got(b, half, 3, mate)
        for n in range(3):
            far_got(b, half, 4 + n, 2 * chips[n] + 1 - core)

    def exchange(ph, src_of, dst_ref):
        for k in range(1, N):
            c = functools.partial(copy, ph, k, src_of(peers[k]), dst_ref.at[me])
            c().start()
            started.append(c)
        dst_ref[me] = src_of(me)[...]

    def arrive(ph, like, dst_ref):
        for k in range(1, N):
            copy(ph, k, like, dst_ref.at[senders[k]]).wait_recv()

    barrier = pltpu.get_barrier_semaphore()
    for k in range(1, N):
        pl.semaphore_signal(barrier, inc=1, device_id={axis: peers[k]}, device_id_type=pl.DeviceIdType.MESH)

    def bias_message(xln, w_bias, heads, msg):
        half = heads // 2
        b = mm(w_bias, xln)
        if heads == 4:
            b = jnp.concatenate([b, b], axis=0)
        bh = pltpu.roll(b, N - half, 0)
        lo = low_lanes(N)
        for i in range(N):
            bl_v = b[:, W * (i // 2):W * (i // 2) + W]
            bh_v = bh[:, W * (i // 2):W * (i // 2) + W]
            if i % 2 == 0:
                pb[N * i:N * i + N, :] = jnp.where(lo, bl_v, pltpu.roll(bh_v, R, 1))
            else:
                pb[N * i:N * i + N, :] = jnp.where(lo, pltpu.roll(bl_v, R, 1), bh_v)
        msg[...] = jnp.concatenate([pb[pl.ds(h, N, stride=N), :] for h in range(half)], axis=0).astype(BF16)

    def bias_table(got, heads, table, gathered_keys):
        half = heads // 2
        full = got[...].astype(F32)
        for h in range(half):
            x = full[:, N * h:N * h + N, :].reshape(R, W)
            if gathered_keys:
                xr = pltpu.roll(x, R, 1)
                lo = low_lanes(R)
                table[R * h:R * h + R, :] = jnp.where(lo, x, xr)
                table[R * (half + h):R * (half + h) + R, :] = jnp.where(lo, xr, x)
            else:
                t = jnp.transpose(x)
                for hp in TWO:
                    blk = t[R * hp:R * hp + R]
                    table[R * (half * hp + h):R * (half * hp + h) + R, :] = jnp.concatenate([blk, blk], axis=1)

    def z_features():
        return jnp.concatenate(
            [jnp.transpose(zst[W * t:W * t + W, :].astype(F32)) for t in FOUR], axis=1)

    need(z_ref, wrb)
    zst[...] = z_ref[...].reshape(T, W)
    bias_message(ln(z_features()), wrb[0], N, bm_r1)
    pl.semaphore_wait(barrier, N - 1)
    exchange(PH_RB1, lambda p: bm_r1, br_r1)

    def fill(ref, fn):
        ref[...] = flag(fn(iota(ref.shape, 0), iota(ref.shape, 1))).astype(BF16)

    def row_constants():
        mt_b = mt_ref[...].astype(F32).astype(BF16)
        sel = (iota((S, W), 0) == Q * me + iota((S, W), 1)) & (iota((S, W), 1) < Q)
        mloc[...] = mm(mt_b, flag(sel).astype(BF16)).astype(BF16)
        fill(hm_r, lambda r, c: r // R == (c % R) // N)
        fill(rm_r, lambda r, c: (r % R) // N == c // R)
        for b in TWO:
            wro_t[b] = jnp.transpose(wro[b].astype(F32)).astype(BF16)

    def far_place(n):
        return (n % H) // 2, 2 * (n % 2) + n // H

    def other_constants():
        mt_b = mt_ref[...].astype(F32).astype(BF16)
        mrows = mt_ref[pl.ds(pl.multiple_of(N * me, N), N), :].astype(F32)
        t = iota((S, S), 1)
        perm = iota((S, S), 0) == (t % R) // N * Q + t // W * H + (t % W) // R * N + t % N
        mp[...] = mm(mrows.astype(BF16), flag(perm).astype(BF16))
        for i in range(N):
            row = jnp.broadcast_to(mrows[i:i + 1, :], (W, S)).astype(BF16)
            rn[i] = 1.0 / (1e-3 + mm_nt(mt_b, row))
        rkey[...] = jnp.transpose(jnp.broadcast_to(r_ref[...].astype(F32), (W, R)))
        fill(hm_t, lambda r, c: r // R == (c % W) // Q)
        fill(rm_t, lambda r, c: (r % W) // Q == c // R)
        for b in TWO:
            wco_t[b] = jnp.transpose(wco[b].astype(F32)).astype(BF16)
            wso_t[b] = jnp.transpose(wso[b].astype(F32)).astype(BF16)
            weo_t[b] = jnp.transpose(weo[b].astype(F32)).astype(BF16)
        wf[...] = woo[0].astype(F32)
        for n in range(Q):
            a, b = far_place(n)
            wall[0, Q * a:Q * a + Q, W * b:W * b + W] = wf[pl.ds(n, Q, stride=Q), :].astype(BF16)

    def row_project(b, load):
        for c in FOUR:
            x = jnp.concatenate([load(4 * c + t) for t in FOUR], axis=1)
            proj = rnd(mm(wri[b], ln(x)))
            for t in FOUR:
                xres[4 * c + t] = x[:, W * t:W * t + W]
                pqm[4 * c + t] = proj[:, W * t:W * t + W]

    def row_loop(lo, hi):
        r, c = iota((W, W), 0), iota((W, W), 1)
        cs = jnp.where(c < R, 0, H)

        def logits(pair, slot):
            sbuf[slot] = pair_logits(pqm[pair, 0:R, :], pqm[pair, R:2 * R, :], N, hm_r)

        def probs(pair, slot):
            key_mask = mm(mloc[...], flag(r == cs + pair).astype(BF16))
            pair_probs(sbuf.at[slot], pbuf.at[slot], N, N, bt_r, key_mask)

        def values(pair, slot):
            obuf[pair] = pair_values(pqm[pair, 2 * R:3 * R, :], pbuf.at[slot], N, rm_r)

        def step(n, carry):
            for t in FOUR:
                p = 4 * n + t
                logits(jnp.minimum(p + 2, 15), (t + 2) % 4)
                probs(p, t)
                values(jnp.maximum(p - 1, 0), (t + 3) % 4)
            return carry

        if lo == 0:
            pbuf[3] = jnp.zeros((T, W), BF16)
            logits(0, 0)
            logits(1, 1)
        lax.fori_loop(lo, hi, step, 0)
        values(4 * hi - 1, 3)

    def row_finish(b, store, chunks):
        for c in chunks:
            g = jnp.concatenate([pqm[4 * c + t, 3 * R:4 * R, :] for t in FOUR], axis=1)
            o = jnp.concatenate([obuf[4 * c + t] for t in FOUR], axis=1)
            x = jnp.concatenate([xres[4 * c + t] for t in FOUR], axis=1)
            y = rnd(x + mm(wro_t[b], gate(o, g)))
            for t in FOUR:
                store(4 * c + t, y[:, W * t:W * t + W])

    need(m_ref, mt_ref, wri, wro)
    row_constants()
    row_project(0, lambda pair: jnp.transpose(jnp.concatenate([m_ref[pair], m_ref[pair + H]], axis=0).astype(F32)))
    arrive(PH_RB1, bm_r1, br_r1)
    bias_table(br_r1, N, bt_r, False)

    def store1(pair, y):
        yt = jnp.transpose(y)
        rowf[R * pair:R * pair + R, :] = jnp.concatenate([yt[0:R], yt[R:W]], axis=1)

    for half in TWO:
        row_loop(2 * half, 2 * half + 2)
        row_finish(0, store1, (2 * half, 2 * half + 1))
        for n in range(Q):
            rows = [rowf[pl.ds(T * half + 2 * n + u, N, stride=R), :] for u in TWO]
            sm1[half, n // 4, n % 4] = jnp.concatenate(rows, axis=0).astype(BF16)
        exchange(PH_M1 + half, lambda p: sm1.at[half, p], rm1.at[half])
    need(r_ref, wci, wco, woi, woo, wsb, wsi, wso, web, wei, weo)
    other_constants()

    def both(ref, i, rows=slice(None)):
        return jnp.concatenate([ref[2 * i, rows, :], ref[2 * i + 1, rows, :]], axis=1)

    def put(ref, i, value):
        ref[2 * i] = value[:, 0:W]
        ref[2 * i + 1] = value[:, W:S]

    def column_project(b, load):
        part = iota((R, S), 0)
        flags = jnp.where(part == 0, NEG_PARTS[0], jnp.where(part == 1, NEG_PARTS[1], jnp.where(part == 2, NEG_PARTS[2], 0.0)))
        for i in range(N):
            x = load(i)
            proj = rnd(mm(wci[b], ln(x)))
            put(xres, i, x)
            put(pqm, i, proj)
            keep = mp[i:i + 1, :]
            ka = jnp.concatenate([proj[R:2 * R] * keep, flags * (1.0 - keep)], axis=0)
            kaug[i] = jnp.transpose(ka).astype(BF16)

    def column_machine():
        head = iota((R, S), 0) // N
        ones = flag(iota((R, S), 0) < 3)

        def logits(i, h, slot):
            q = jnp.where(head == h, both(pqm, i, slice(0, R)), 0.0)
            s = mm(kaug[i], jnp.concatenate([q, ones], axis=0).astype(BF16))
            sbuf[slot, 0:S, :] = s[:, 0:W]
            sbuf[slot, S:2 * S, :] = s[:, W:S]

        def probs(slot):
            for n in TWO:
                rows = slice(S * n, S * n + S)
                pbuf[slot, rows, :] = softmax_keys(sbuf[slot, rows, :], N ** -0.5 * LOG2E)

        def values(i, h, slot):
            rows = slice(2 * R + N * h, 2 * R + N * h + N)
            vh = both(pqm, i, rows).astype(BF16)
            p = jnp.concatenate([pbuf[slot, 0:S, :], pbuf[slot, S:2 * S, :]], axis=1)
            o = mm(vh, p)
            obuf[2 * i, N * h:N * h + N, :] = o[:, 0:W]
            obuf[2 * i + 1, N * h:N * h + N, :] = o[:, W:S]

        def begin():
            pbuf[3] = jnp.zeros((T, W), BF16)
            logits(0, 0, 0)
            logits(0, 1, 1)

        def loop(lo, hi, at=None, event=None):
            def step(i, carry):
                if event is not None:
                    pl.when(i == at)(event)
                later = jnp.minimum(i + 1, 7)
                for h in range(N):
                    logits(i if h < 6 else later, (h + 2) % N, (h + 2) % 4)
                    probs(h % 4)
                    values(jnp.maximum(i - 1, 0) if h == 0 else i, (h + 7) % N, (h + 3) % 4)
                return carry

            lax.fori_loop(lo, hi, step, 0)

        return begin, loop, lambda i: values(i, 7, 3)

    column_begin, column_loop, column_drain = column_machine()

    def column_finish(b, half, finish):
        column_drain(4 * half + 3)
        for i in range(4 * half, 4 * half + 4):
            y = rnd(both(xres, i) + mm(wco_t[b], gate(both(obuf, i), both(pqm, i, slice(3 * R, 4 * R)))))
            finish(i, y)
        pack_far(b, half)

    def opm_operands(b, xt, i):
        proj = mm(woi[b], ln(xt)) * mp[i:i + 1, :]
        near, far = (proj[0:Q], proj[Q:R]) if b == 0 else (proj[Q:R], proj[0:Q])
        rows = slice(Q * i, Q * i + Q)
        aloc[b, rows, :] = near.astype(BF16)
        for qh in TWO:
            at = W * (i // 4) + H * (4 * qh + i % 4)
            for t in TWO:
                remf[t, at:at + H, :] = far[H * qh:H * qh + H, W * t:W * t + W]

    def pack_far(b, half):
        for n in range(N):
            for t in TWO:
                at = W * half + H * n
                rem[b, at:at + H, W * t:W * t + W] = jnp.concatenate(
                    [remf[t, pl.ds(W * half + 2 * n + u, N, stride=H), :] for u in TWO], axis=0).astype(BF16)

    for half in TWO:
        arrive(PH_M1 + half, sm1.at[half, 0], rm1.at[half])

    def load1(i):
        rows = slice(N * (i % 2), N * (i % 2) + N)
        xt = jnp.transpose(jnp.concatenate(
            [rm1[half, :, i // 2].astype(F32)[:, rows, :].reshape(R, W) for half in TWO], axis=0))
        return jnp.concatenate([xt[0:R], xt[R:W]], axis=1)

    def finish1(i, y):
        m1[i] = y.astype(BF16)
        opm_operands(0, y, i)

    column_project(0, load1)
    column_begin()
    for half in TWO:
        column_loop(4 * half, 4 * half + 4)
        column_finish(0, half, finish1)
        far_start(0, half, FOUR)
    cg[0, me] = rem[0]

    def finish2(i, y):
        opm_operands(1, y, i)
        yt = jnp.transpose(jnp.concatenate([y[:, 0:W], y[:, W:S]], axis=0)).reshape(2, N, N, W)
        sm2[:, i] = jnp.concatenate([yt[0], yt[1]], axis=1).astype(BF16)

    column_project(1, lambda i: m1[i].astype(F32))
    column_begin()
    column_loop(0, 4, 1, lambda: far_forward(0, 0, range(3)))
    column_finish(1, 0, finish2)
    far_start(1, 0, FOUR)
    column_loop(4, 6, 5, lambda: far_forward(0, 1, range(3)))

    def opm(b):
        for half in TWO:
            far_arrive(b, half)
        for n in range(N):
            far = jnp.concatenate(
                [cg[b, :, W * half + H * n:W * half + H * n + H, :].reshape(W, S) for half in TWO], axis=0)
            o = mm_nt(aloc[b], far).astype(BF16)
            for i in range(N):
                xop[i, Q * n:Q * n + Q, :] = o[Q * i:Q * i + Q, :]
        first = iota((1, 1, N, W), 2) < 4
        for i in range(N):
            y = mm(jnp.transpose(xop[i]), wall[b]).reshape(2, N, 2, N, T)
            u = sum(jnp.where(first, y[:, :, n, :, 2 * W * n:2 * W * n + W], y[:, :, n, :, 2 * W * n + W:2 * W * n + 2 * W])
                    for n in TWO)
            u = (u.reshape(H, N, W) + pltpu.roll(u.reshape(H, N, W), 4, 1)).reshape(2, N, N, W)
            u = jnp.where(first[0], u[0], u[1]).reshape(R, W)
            rows = slice(R * i, R * i + R)
            zst[rows, :] = (zst[rows, :].astype(F32) + u * rn[i]).astype(BF16)

    def tri_part(n, t):
        return pq[W * n:W * n + W, W * t:W * t + W]

    def tri_logits(xln, w_in):
        pq[...] = rnd(mm(w_in, xln))
        for t in FOUR:
            stri[t] = pair_logits(tri_part(0, t), tri_part(1, t), 4, hm_t)

    def tri_attend(x, w_out_t):
        for t in FOUR:
            pair_probs(stri.at[t], ptri.at[t], 4, Q, bt_t, rkey[...])
        o = jnp.concatenate([pair_values(tri_part(2, t), ptri.at[t], 4, rm_t) for t in FOUR], axis=1)
        return rnd(x + mm(w_out_t, gate(o, pq[3 * W:4 * W, :])))

    def swap_pair(y, n):
        for t in FOUR:
            zf[W * t:W * t + W, :] = jnp.transpose(y[:, W * t:W * t + W])
        for c in range(Q):
            sz[n, H * c:H * c + H, :] = jnp.concatenate(
                [zf[pl.ds(2 * c, N, stride=R), :], zf[pl.ds(2 * c + 1, N, stride=R), :]], axis=0).astype(BF16)

    def take_pair(n):
        x = rz[n].astype(F32).reshape(N, N, N, W)
        for j in range(N):
            zst[R * j:R * j + R, :] = x[:, j].reshape(R, W).astype(BF16)

    def z_block(n, p):
        return sz.at[n, pl.ds(pl.multiple_of(R * p, R), R), :]

    opm(0)
    x = z_features()
    xln = ln(x)
    bias_message(xln, wsb[0], 4, bm_s1)
    exchange(PH_SB1, lambda p: bm_s1, br_s1)
    tri_logits(xln, wsi[0])
    column_loop(6, N)
    column_finish(1, 1, finish2)
    far_start(1, 1, (0, 1, 3))
    cg[1, me] = rem[1]
    arrive(PH_SB1, bm_s1, br_s1)
    bias_table(br_s1, 4, bt_t, False)
    y = tri_attend(x, wso_t[0])
    swap_pair(y, 0)
    exchange(PH_Z1, lambda p: z_block(0, p), rz.at[0])
    bias_message(ln(y), web[0], 4, bm_e1)
    exchange(PH_EB1, lambda p: bm_e1, br_e1)
    far_start(1, 1, (2,))
    exchange(PH_M2, lambda p: sm2.at[p], rm2)
    far_forward(1, 0, range(3))
    far_forward(1, 1, TWO)
    for n in range(Q):
        a, b = far_place(n)
        wall[1, Q * a:Q * a + Q, W * b:W * b + W] = woo[1, Q * n:Q * n + Q, :]
    arrive(PH_Z1, z_block(0, 0), rz.at[0])
    take_pair(0)
    x = z_features()
    tri_logits(ln(x), wei[0])
    arrive(PH_EB1, bm_e1, br_e1)
    bias_table(br_e1, 4, bt_t, True)
    y = tri_attend(x, weo_t[0])
    far_forward(1, 1, (2,))
    bias_message(ln(y), wrb[1], N, bm_r2)
    exchange(PH_RB2, lambda p: bm_r2, br_r2)
    for t in FOUR:
        zst[W * t:W * t + W, :] = jnp.transpose(y[:, W * t:W * t + W]).astype(BF16)

    opm(1)
    x = z_features()
    xln = ln(x)
    bias_message(xln, web[1], 4, bm_e2)
    exchange(PH_EB2, lambda p: bm_e2, br_e2)
    tri_logits(xln, wei[1])

    arrive(PH_M2, sm2.at[0], rm2)
    rowf[...] = rm2[...].reshape(1024, W).astype(F32)

    def load2(pair):
        xt = jnp.transpose(rowf[pl.ds(pair, R, stride=H), :])
        return jnp.concatenate([xt[0:R], xt[R:W]], axis=1)

    def store2(pair, y):
        mst[pair] = y.astype(BF16)

    row_project(1, load2)
    arrive(PH_RB2, bm_r2, br_r2)
    bias_table(br_r2, N, bt_r, True)
    row_loop(0, 2)

    arrive(PH_EB2, bm_e2, br_e2)
    bias_table(br_e2, 4, bt_t, False)
    y = tri_attend(x, weo_t[1])
    swap_pair(y, 1)
    exchange(PH_Z2, lambda p: z_block(1, p), rz.at[1])
    bias_message(ln(y), wsb[1], 4, bm_s2)
    exchange(PH_SB2, lambda p: bm_s2, br_s2)
    row_loop(2, 4)
    row_finish(1, store2, FOUR)
    m_copy = pltpu.make_async_copy(mst, mo_ref, load_sem.at[17])
    m_copy.start()
    arrive(PH_Z2, z_block(1, 0), rz.at[1])
    take_pair(1)
    x = z_features()
    tri_logits(ln(x), wsi[1])
    arrive(PH_SB2, bm_s2, br_s2)
    bias_table(br_s2, 4, bt_t, True)
    y = tri_attend(x, wso_t[1])
    for t in FOUR:
        zo_ref[W * t:W * t + W, :] = jnp.transpose(y[:, W * t:W * t + W]).astype(BF16)

    m_copy.wait()
    for c in started:
        c().wait_send()


def unpack(y_ref, z_ref, mo_ref, zo_ref):
    for pair in range(y_ref.shape[0]):
        yt = jnp.transpose(y_ref[pair].astype(F32)).astype(BF16)
        mo_ref[0, pair] = yt[0:R]
        mo_ref[1, pair] = yt[R:W]
    zo_ref[...] = z_ref[...].reshape(zo_ref.shape)


def solution(mesh):
    axis, steps = 'dap', 4

    def local_step(m, z, msa_mask, res_mask, w_row_bias, w_row_in, w_row_out, w_col_in, w_col_out, w_opm_in, w_opm_out,
                   w_ts_bias, w_ts_in, w_ts_out, w_te_bias, w_te_in, w_te_out):
        def tin(w):
            return jnp.moveaxis(w, 1, -1).reshape(2, -1, w.shape[1])

        args = (m, z, msa_mask.T, res_mask[None, :],
                tin(w_row_bias), tin(w_row_in), w_row_out.reshape(2, R, R), tin(w_col_in), w_col_out.reshape(2, R, R),
                tin(w_opm_in), w_opm_out.reshape(2, 1024, W),
                tin(w_ts_bias), tin(w_ts_in), w_ts_out.reshape(2, W, W),
                tin(w_te_bias), tin(w_te_in), w_te_out.reshape(2, W, W))
        v = pltpu.VMEM
        scratch = [v(a.shape, a.dtype) for a in args] + [
            pltpu.SemaphoreType.DMA((18,)),
            v((N, S), F32), v((R, W), BF16), v((N, R, W), F32), v((R, W), F32),
            v((T, W), BF16), v((W, T), BF16), v((S, S), BF16), v((S, S), BF16),
            v((2, R, R), BF16), v((2, R, R), BF16), v((2, W, W), BF16), v((2, W, W), BF16),
            v((2, S, T), BF16), v((1024, W), F32),
            v((1024, W), F32), v((2, N, 4, H, W), BF16), v((2, N, 4, H, W), BF16), v((N, R, S), BF16),
            v((N, N, H, W), BF16), v((N, N, H, W), BF16),
            v((2, S, S), BF16), v((2, S, W), F32), v((2, S, S), BF16), v((2, N, S, S), BF16), v((N, S, S), BF16),
            v((T, W), BF16), v((T, W), F32), v((2, T, W), BF16), v((2, N, R, W), BF16), v((R, W), F32),
            v((Q, W), BF16), v((Q, W), BF16), v((N, Q, W), BF16), v((N, Q, W), BF16),
            v((H, W), BF16), v((H, W), BF16), v((H, W), BF16), v((H, W), BF16),
            v((N, H, W), BF16), v((N, H, W), BF16), v((N, H, W), BF16), v((N, H, W), BF16),
            v((T, W), F32), v((S, W), F32), v((T, T), F32),
            v((4, T, W), F32), v((4, T, W), BF16), v((H, S, W), F32), v((H, R, W), F32), v((H, R, W), F32), v((N, S, W), BF16), v((4, S, W), F32), v((4, S, W), BF16), v((H, R, W), BF16),
            pltpu.SemaphoreType.DMA((H, N)), pltpu.SemaphoreType.DMA((H, N)),
        ]
        vmem = pl.BlockSpec(memory_space=pltpu.VMEM)
        mo, zo = pl.pallas_call(
            functools.partial(kernel, axis),
            out_shape=(jax.ShapeDtypeStruct((H, R, W), BF16), jax.ShapeDtypeStruct((T, W), BF16)),
            in_specs=[pl.BlockSpec(memory_space=pltpu.HBM)] * len(args),
            out_specs=(pl.BlockSpec(memory_space=pltpu.HBM), vmem),
            scratch_shapes=scratch,
            compiler_params=pltpu.CompilerParams(collective_id=0, has_side_effects=True, vmem_limit_bytes=60 * 1024 * 1024),
        )(*args)
        mo, zo = pl.pallas_call(
            unpack,
            grid=(steps,),
            out_shape=(jax.ShapeDtypeStruct((2, H, R, R), BF16), jax.ShapeDtypeStruct((N, R, W), BF16)),
            in_specs=[pl.BlockSpec((H // steps, R, W), lambda i: (i, 0, 0)), pl.BlockSpec((T // steps, W), lambda i: (i, 0))],
            out_specs=(pl.BlockSpec((2, H // steps, R, R), lambda i: (0, i, 0, 0)),
                       pl.BlockSpec((N // steps, R, W), lambda i: (i, 0, 0))),
        )(mo, zo)
        return mo.reshape(Q, R, R), zo

    in_specs = (P(('data', 'dap')), P(('data', 'dap')), P('data'), P('data')) + (P(),) * 13
    out_specs = (P(('data', 'dap')), P(('data', 'dap')))
    return jax.shard_map(local_step, mesh=mesh, in_specs=in_specs, out_specs=out_specs, check_vma=False)
```
